128 devices in a mesh: grp: 8 (over x_lo, z), loc: 16 (over y, x_hi, core).
Axes of the slice: x: 4 (x_hi: 2, x_lo: 2; x = x_hi * 2 + x_lo), y: 4, z: 4, core: 2. Of those that a mesh axis runs over, the one named last changes fastest.
Arguments:
- features: float32 [131072, 256], P(('grp', 'loc')), may hold values from -6 to 6
- hub_block: bfloat16 [512, 131072], P(None, ('grp', 'loc')), may hold values from -0.0625 to 0.0625
- hub_slot: int32 [512], P(('grp', 'loc')), may hold values from 0 to 1023, as said below
- neighbours: int32 [131072, 16], P(('grp', 'loc')), may hold values from 0 to 3071
- counts: int32 [131072], P(('grp', 'loc')), may hold values from 1 to 16
- halo_send: int32 [2048, 128], P(('grp', 'loc')), may hold values from 0 to 1023
- weight: float32 [256, 256], replicated, may hold values from -0.375 to 0.375
- bias: float32 [256], replicated, may hold values from -3 to 3
Outputs:
- layer_out: float32 [131072, 256], P(('grp', 'loc'))
The draws below stay inside these ranges and needn't reach their ends.
Inputs may be any that keep to these rules, and one draw needn't show every extreme that they name: `hub_slot`: within each aligned block of 4 entries the values are distinct.
All inputs are finite; a program needn't handle non-finite values.
Results may differ from the reference program's by a relative error of at most 0.0003.
Values sent between devices are 32-bit elements; how exact they have to be, the bound alone decides.
A program may use at most 64 MiB of HBM per device.

```python
import jax
import jax.numpy as jnp
from jax import lax

F = 256
V_DEV = 1024
HUB_DEV = 4
K = 16
S = 128
V = 131072
HUB = 512
N_GRP = 8
N_LOC = 16
DEVICES = 128


def draw_hub_slot(key, part):
    owners = HUB // HUB_DEV
    keys = jax.random.split(jax.random.fold_in(key, 11), owners)
    picked = jax.vmap(lambda single: jax.random.permutation(single, V_DEV)[:HUB_DEV])(keys)
    return picked.reshape(-1).astype(jnp.int32)


def place_ends(array, stream_key, least, largest):
    shape = array.shape
    spot = [jax.random.randint(jax.random.fold_in(stream_key, axis), (), 0, shape[axis]) for axis in range(len(shape))]
    array = array.at[tuple(spot)].set(least)
    longest = shape.index(max(shape))
    spot[longest] = (spot[longest] + 1) % shape[longest]
    return array.at[tuple(spot)].set(largest)


def spiked(entries, own_key, source, target, blocks, factor):
    def block_of(position):
        return (jnp.arange(entries.shape[position]) // (entries.shape[position] // blocks)).reshape((-1,) + (1,) * (entries.ndim - 1 - position))

    first = jax.random.permutation(own_key, blocks)[block_of(target)]
    other_side = (block_of(target) + blocks // 2) % blocks
    return jnp.where((block_of(source) == first) | (block_of(source) == other_side), factor * entries, entries)


def block_levels(key, extent, cuts, low, top_value):
    def one(dim, shards_of):
        draws = jax.random.uniform(jax.random.fold_in(jax.random.fold_in(key, 6), dim), (shards_of,), jnp.float32, low / len(cuts), top_value / len(cuts))
        return jnp.repeat(jnp.exp(draws), extent[dim] // shards_of).reshape((-1,) + (1,) * (len(extent) - dim - 1))

    loudness = one(*cuts[0])
    for cut in cuts[1:]:
        loudness = loudness * one(*cut)
    return loudness


def centred(key, extent, width, bound, cuts=(), kind=jnp.bfloat16):
    array = jax.random.normal(key, extent, jnp.float32) * width
    if len(cuts) > 0:
        array = block_levels(key, extent, cuts, -0.22, 0.18) * array
    return jnp.clip(array, min=-bound, max=bound).astype(kind)


def heavy_noise(key, extent, deviation, most, cuts, heavy, kind=jnp.bfloat16):
    entries = deviation * jax.random.normal(key, extent, jnp.float32)
    if cuts:
        entries = entries * block_levels(key, extent, cuts, -0.22, 0.18)
    return jnp.clip(spiked(entries, jax.random.fold_in(key, 3), *heavy), -most, most).astype(kind)


def setup_inputs(seed: int = 0) -> dict:
    splits = jax.random.split(jax.random.key(seed), 9)
    return {
        "features": centred(splits[0], (V, F), 1.0, 6.0, ((0, 128),), jnp.float32),
        "hub_block": heavy_noise(splits[1], (HUB, V), V ** -0.5, 0.0625, ((1, 128),), (1, 0, 128, 5.5)),
        "hub_slot": draw_hub_slot(jax.random.fold_in(splits[8], 71), 0),
        "neighbours": place_ends(jax.random.randint(splits[3], (V, K), 0, V_DEV + N_LOC * S), jax.random.fold_in(splits[3], 1), 0, (V_DEV + N_LOC * S) - 1).astype(jnp.int32),
        "counts": place_ends(jax.random.randint(splits[4], (V,), 1, K + 1), jax.random.fold_in(splits[4], 1), 1, K).astype(jnp.int32),
        "halo_send": place_ends(jax.random.randint(splits[5], (DEVICES * N_LOC, S), 0, V_DEV), jax.random.fold_in(splits[5], 1), 0, V_DEV - 1).astype(jnp.int32),
        "weight": centred(splits[6], (F, F), F ** -0.5, 0.375, (), jnp.float32),
        "bias": centred(splits[7], (F,), 0.5, 3.0, (), jnp.float32),
    }


def reference(features, hub_block, hub_slot, neighbours, counts, halo_send, weight, bias):
    rounded = features.astype(jnp.bfloat16)
    hub_sum = jnp.dot(hub_block, rounded, preferred_element_type=jnp.float32)
    devices = N_GRP * N_LOC
    send_table = halo_send.reshape(devices, N_LOC, S)
    nbr_blocks = neighbours.reshape(devices, V_DEV, K)
    cnt_blocks = counts.reshape(devices, V_DEV)

    def one_device(device):
        group = device // N_LOC
        place = device % N_LOC
        peers = (group * N_LOC + jnp.arange(N_LOC)).astype(jnp.int32)
        sent_rows = send_table[peers, place]
        remote_ids = (peers[:, None] * V_DEV + sent_rows).reshape(-1)
        own_ids = (device * V_DEV + jnp.arange(V_DEV)).astype(jnp.int32)
        ids_table = jnp.concatenate([own_ids, remote_ids.astype(jnp.int32)])
        slots = nbr_blocks[device]
        gathered = features[ids_table[slots]]
        used = (jnp.arange(K)[None, :] < cnt_blocks[device][:, None]).astype(jnp.float32)
        summed = jnp.sum(gathered * used[:, :, None], axis=1)
        return summed / cnt_blocks[device].astype(jnp.float32)[:, None]

    low = lax.map(one_device, jnp.arange(devices).astype(jnp.int32)).reshape(-1, F)
    combined = features + low
    targets = (jnp.arange(HUB) // HUB_DEV).astype(jnp.int32) * V_DEV + hub_slot
    combined = combined.at[targets].add(hub_sum)
    result = jnp.dot(combined, weight, precision=lax.Precision.HIGHEST, preferred_element_type=jnp.float32) + bias
    return jnp.maximum(result, 0.0)
```

```python
import jax
import jax.numpy as jnp
from jax import lax
from jax.experimental import pallas as pl
from jax.experimental.pallas import tpu as pltpu
from jax.sharding import PartitionSpec as P

MESH = pl.DeviceIdType.MESH
NY, NXH, NC, NXL, NZ = 4, 2, 2, 2, 4
ROWS, WIDTH, SLOTS, SENT = 1024, 256, 16, 128
HUBS, HUB_OWN = 512, 4
FIELD_ROWS, FIELDS, FIELD_BITS = 512, 6, 5
CHUNK = 256

SEND_ORDER = (
    (2, 1, 0), (1, 0, 0), (3, 0, 0), (0, 1, 0),
    (1, 1, 1), (3, 1, 1), (2, 0, 1), (0, 1, 1),
    (1, 1, 0), (3, 1, 0), (2, 0, 0), (2, 1, 1),
    (1, 0, 1), (3, 0, 1), (0, 0, 1), (0, 0, 0),
)
TAKE_ORDER = ((0, 0), (0, 1), (2, 0), (2, 1), (1, 1), (3, 1), (1, 0), (3, 0))


def split2(value):
    high = value.astype(jnp.bfloat16)
    low = (value - high.astype(jnp.float32)).astype(jnp.bfloat16)
    return high, low


def mm(left, right):
    return jnp.dot(left, right, preferred_element_type=jnp.float32)


def kernel(
    feat_hbm, hub_hbm, slot_hbm, nbr_hbm, cnt_hbm, halo_hbm, weight_hbm, bias_hbm,
    out_ref,
    feat, hub, slot, nbr, cnt, halo, weight, bias,
    fhi, flo, halo_rel, one_hot, stage, recv,
    part, part_in, pair_sum, z_in, z_sum, plane_in,
    marks, recip, adjacency, total, w_hi, w_lo,
    in_sem, halo_send, halo_recv, a_sem, b_send, b_recv, c_send, c_recv,
):
    g, l = lax.axis_index("grp"), lax.axis_index("loc")
    y, xh, c = l // 4, (l // 2) % 2, l % 2
    xl, z = g // 4, g % 4
    x = xh * 2 + xl

    def loc_of(dy, dx, dc):
        return ((y + dy) % NY) * 4 + ((xh + dx) % NXH) * 2 + (c + dc) % NC

    def plane_of(dx, dy):
        tx, ty = (x + dx) % 4, (y + dy) % NY
        return (tx % 2) * 4 + z, ty * 4 + (tx // 2) * 2 + c

    loads = []
    for number, (source, target) in enumerate((
        (feat_hbm, feat), (halo_hbm, halo), (hub_hbm, hub), (nbr_hbm, nbr),
        (cnt_hbm, cnt), (weight_hbm, weight), (bias_hbm, bias), (slot_hbm, slot),
    )):
        copy = pltpu.make_async_copy(source, target, in_sem.at[number])
        copy.start()
        loads.append(copy)

    barrier = pltpu.get_barrier_semaphore()
    greeted = 0
    for step in SEND_ORDER:
        if step != (0, 0, 0):
            pl.semaphore_signal(barrier, inc=1, device_id=(g, loc_of(*step)), device_id_type=MESH)
            greeted += 1
    for dz in range(1, NZ):
        pl.semaphore_signal(
            barrier, inc=1, device_id=(xl * 4 + (z + dz) % NZ, l), device_id_type=MESH
        )
        greeted += 1
    for dx in (1, 3):
        for dy in range(NY):
            pl.semaphore_signal(barrier, inc=1, device_id=plane_of(dx, dy), device_id_type=MESH)
            greeted += 1

    loads[1].wait()
    for number, step in enumerate(SEND_ORDER):
        halo_rel[number : number + 1, :] = halo[pl.ds(loc_of(*step), 1), :]
    columns = halo_rel[...].T
    loads[0].wait()
    for start in range(0, ROWS, 256):
        high, low = split2(feat[start : start + 256, :])
        fhi[start : start + 256, :] = high
        flo[start : start + 256, :] = low
    lane = lax.broadcasted_iota(jnp.int32, (SENT, ROWS), 1)
    halo_copies = {}
    for group in range(4):
        for inner in range(4):
            number = group * 4 + inner
            one_hot[inner * SENT : (inner + 1) * SENT, :] = jnp.where(
                lane == columns[:, number : number + 1], 1.0, 0.0
            ).astype(jnp.bfloat16)
        rows = mm(one_hot[...], fhi[...]) + mm(one_hot[...], flo[...])
        for inner in range(4):
            number = group * 4 + inner
            step = SEND_ORDER[number]
            block = rows[inner * SENT : (inner + 1) * SENT, :]
            place = step[0] * NXH + step[1]
            if step == (0, 0, 0):
                recv[place, pl.ds(c, 1)] = block[None]
            else:
                stage[number] = block
        if group == 0:
            pl.semaphore_wait(barrier, greeted)
        for inner in range(4):
            number = group * 4 + inner
            step = SEND_ORDER[number]
            if step != (0, 0, 0):
                copy = pltpu.make_async_remote_copy(
                    src_ref=stage.at[number],
                    dst_ref=recv.at[step[0] * NXH + step[1], c],
                    send_sem=halo_send.at[number],
                    recv_sem=halo_recv.at[number],
                    device_id=(g, loc_of(*step)),
                    device_id_type=MESH,
                )
                copy.start()
                halo_copies[step] = copy

    loads[2].wait()
    upper = lax.broadcasted_iota(jnp.int32, (128, 128), 0) % 8 < 4
    for start in range(0, HUBS, 128):
        rows = mm(hub[start : start + 128, :], fhi[...])
        left, right = rows[:, :128], rows[:, 128:]
        part[0, start : start + 128, :] = jnp.where(upper, left, pltpu.roll(right, 4, 0))
        part[1, start : start + 128, :] = jnp.where(upper, pltpu.roll(left, 124, 0), right)
    pair_copy = pltpu.make_async_remote_copy(
        src_ref=part.at[1 - c],
        dst_ref=part_in,
        send_sem=a_sem.at[0],
        recv_sem=a_sem.at[1],
        device_id=(g, loc_of(0, 0, 1)),
        device_id_type=MESH,
    )
    pair_copy.start()

    loads[3].wait()
    loads[4].wait()
    slots, used = nbr[...], cnt[...]
    active = lax.broadcasted_iota(jnp.int32, (SLOTS, ROWS), 0) < used
    place = slots & (FIELD_ROWS - 1)
    one = jnp.where(active, jnp.left_shift(1, (slots >> 9) * FIELD_BITS), 0)
    inverse = jnp.broadcast_to(1.0 / used.astype(jnp.float32), (8, ROWS))
    for start in range(0, ROWS, 128):
        rows = slice(start, start + 128)
        marks[0, rows, :] = place[:, rows].T
        marks[1, rows, :] = one[:, rows].T
        recip[rows, :] = inverse[:, rows].T

    pool_lane = lax.broadcasted_iota(jnp.int32, (32, FIELD_ROWS), 1)

    def build(block, carry):
        rows = pl.ds(pl.multiple_of(block * 32, 32), 32)
        row_place, row_one = marks[0, rows, :], marks[1, rows, :]
        packed = jnp.zeros((32, FIELD_ROWS), jnp.int32)
        for k in range(SLOTS):
            packed = packed + jnp.where(
                row_place[:, k : k + 1] == pool_lane, row_one[:, k : k + 1], 0
            )
        for field in range(FIELDS):
            number = (packed >> (field * FIELD_BITS)) & (2**FIELD_BITS - 1)
            number = number.astype(jnp.float32).astype(jnp.bfloat16)
            adjacency[2 * field, rows, :] = number[:, :CHUNK]
            adjacency[2 * field + 1, rows, :] = number[:, CHUNK:]
        return carry

    lax.fori_loop(0, 8, build, 0)

    pair_copy.wait_recv()
    own = pl.ds(c, 1)
    pair_sum[...] = (part[own][0] + part_in[...]).reshape(NXL, NZ, 64, 128)
    z_copies = []
    for dz in range(1, NZ):
        to = (z + dz) % NZ
        copy = pltpu.make_async_remote_copy(
            src_ref=pair_sum.at[:, to],
            dst_ref=z_in.at[dz - 1],
            send_sem=b_send.at[dz - 1],
            recv_sem=b_recv.at[dz - 1],
            device_id=(xl * 4 + to, l),
            device_id_type=MESH,
        )
        copy.start()
        z_copies.append(copy)

    lax.fori_loop(8, 24, build, 0)

    for copy in z_copies:
        copy.wait_recv()
    for half in range(NXL):
        value = pair_sum[half, pl.ds(z, 1)][0]
        for dz in range(NZ - 1):
            value = value + z_in[dz, half]
        z_sum[half] = value.reshape(8, 8, 128)
    plane_copies = []
    for dx in range(4):
        for dy in range(NY):
            if (dx, dy) == (0, 0):
                continue
            tx, ty = (x + dx) % 4, (y + dy) % NY
            copy = pltpu.make_async_remote_copy(
                src_ref=z_sum.at[tx % 2, ty * 2 + tx // 2],
                dst_ref=plane_in.at[dx * 4 + dy],
                send_sem=c_send.at[dx * 4 + dy],
                recv_sem=c_recv.at[dx * 4 + dy],
                device_id=plane_of(dx, dy),
                device_id_type=MESH,
            )
            copy.start()
            plane_copies.append(copy)

    lax.fori_loop(24, 32, build, 0)

    for number in range(4):
        rows = slice(number * CHUNK, (number + 1) * CHUNK)
        value = mm(adjacency[number], fhi[rows, :]) + mm(adjacency[number], flo[rows, :])
        total[...] = value if number == 0 else total[...] + value

    loads[5].wait()
    loads[6].wait()
    loads[7].wait()
    w_hi[...], w_lo[...] = split2(weight[...])

    for number, (dy, dx) in enumerate(TAKE_ORDER):
        for dc in range(NC):
            if (dy, dx, dc) != (0, 0, 0):
                halo_copies[(dy, dx, dc)].wait_recv()
        chip = ((y + NY - dy) % NY) * 2 + (xh + NXH - dx) % NXH
        high, low = split2(recv[dy * NXH + dx].reshape(CHUNK, WIDTH))
        links = adjacency[pl.ds(4 + chip, 1)][0]
        total[...] += mm(links, high) + mm(links, low)

    for copy in plane_copies:
        copy.wait_recv()
    hub_tile = z_sum[pl.ds(xl, 1), pl.ds(y * 2 + xh, 1)][0, 0]
    for number in range(1, 16):
        hub_tile = hub_tile + plane_in[number]
    for start in range(0, ROWS, 256):
        rows = slice(start, start + 256)
        index = lax.broadcasted_iota(jnp.int32, (256, WIDTH), 0) + start
        hub_add = jnp.zeros((256, WIDTH), jnp.float32)
        for r in range(HUB_OWN):
            row = jnp.concatenate([hub_tile[r : r + 1, :], hub_tile[4 + r : 5 + r, :]], axis=1)
            hub_add = jnp.where(index == slot[r], row, hub_add)
        combined = feat[rows, :] + total[rows, :] * recip[rows, 0:1] + hub_add
        high, low = split2(combined)
        value = mm(high, w_hi[...]) + mm(low, w_hi[...]) + mm(high, w_lo[...]) + bias[...]
        out_ref[rows, :] = jnp.maximum(value, 0.0)

    for copy in halo_copies.values():
        copy.wait_send()
    pair_copy.wait_send()
    for copy in z_copies + plane_copies:
        copy.wait_send()


def on_device(features, hub_block, hub_slot, neighbours, counts, halo_send, weight, bias):
    f32, bf16, i32 = jnp.float32, jnp.bfloat16, jnp.int32
    vmem, dma = pltpu.VMEM, pltpu.SemaphoreType.DMA
    return pl.pallas_call(
        kernel,
        out_shape=jax.ShapeDtypeStruct((ROWS, WIDTH), f32),
        in_specs=[pl.BlockSpec(memory_space=pltpu.HBM)] * 8,
        out_specs=pl.BlockSpec(memory_space=pltpu.VMEM),
        scratch_shapes=[
            vmem((ROWS, WIDTH), f32),
            vmem((HUBS, ROWS), bf16),
            pltpu.SMEM((HUB_OWN,), i32),
            vmem((SLOTS, ROWS), i32),
            vmem((1, ROWS), i32),
            vmem((16, SENT), i32),
            vmem((WIDTH, WIDTH), f32),
            vmem((1, WIDTH), f32),
            vmem((ROWS, WIDTH), bf16),
            vmem((ROWS, WIDTH), bf16),
            vmem((16, SENT), i32),
            vmem((4 * SENT, ROWS), bf16),
            vmem((16, SENT, WIDTH), f32),
            vmem((8, NC, SENT, WIDTH), f32),
            vmem((NC, HUBS, 128), f32),
            vmem((HUBS, 128), f32),
            vmem((NXL, NZ, 64, 128), f32),
            vmem((NZ - 1, NXL, 64, 128), f32),
            vmem((NXL, 8, 8, 128), f32),
            vmem((16, 8, 128), f32),
            vmem((2, ROWS, SLOTS), i32),
            vmem((ROWS, 8), f32),
            vmem((2 * FIELDS, ROWS, CHUNK), bf16),
            vmem((ROWS, WIDTH), f32),
            vmem((WIDTH, WIDTH), bf16),
            vmem((WIDTH, WIDTH), bf16),
            dma((8,)), dma((16,)), dma((16,)), dma((2,)),
            dma((3,)), dma((3,)), dma((16,)), dma((16,)),
        ],
        compiler_params=pltpu.CompilerParams(
            collective_id=0, has_side_effects=True, vmem_limit_bytes=40 * 1024 * 1024
        ),
    )(
        features, hub_block, hub_slot, neighbours.T, counts.reshape(1, -1), halo_send,
        weight, bias.reshape(1, -1),
    )


def solution(mesh):
    in_specs = (
        P(("grp", "loc"), None),
        P(None, ("grp", "loc")),
        P(("grp", "loc")),
        P(("grp", "loc"), None),
        P(("grp", "loc")),
        P(("grp", "loc"), None),
        P(),
        P(),
    )
    out_specs = P(("grp", "loc"), None)
    return jax.shard_map(
        on_device, mesh=mesh, in_specs=in_specs, out_specs=out_specs, check_vma=False
    )
```

```python
import jax
import jax.numpy as jnp
from jax import lax
from jax.experimental import pallas as pl
from jax.experimental.pallas import tpu as pltpu
from jax.sharding import PartitionSpec as P

MESH = pl.DeviceIdType.MESH
NY, NXH, NC, NXL, NZ = 4, 2, 2, 2, 4
ROWS, WIDTH, SLOTS, SENT = 1024, 256, 16, 128
HUBS, HUB_OWN = 512, 4
FIELD_ROWS, FIELDS, FIELD_BITS = 512, 6, 5
CHUNK = 256

SEND_ORDER = (
    (2, 1, 0), (1, 0, 0), (3, 0, 0), (0, 1, 0),
    (1, 1, 1), (3, 1, 1), (2, 0, 1), (0, 1, 1),
    (1, 1, 0), (3, 1, 0), (2, 0, 0), (2, 1, 1),
    (1, 0, 1), (3, 0, 1), (0, 0, 1), (0, 0, 0),
)
TAKE_ORDER = ((0, 0), (0, 1), (2, 0), (2, 1), (1, 1), (3, 1), (1, 0), (3, 0))


def split2(value):
    high = value.astype(jnp.bfloat16)
    low = (value - high.astype(jnp.float32)).astype(jnp.bfloat16)
    return high, low


def mm(left, right):
    return jnp.dot(left, right, preferred_element_type=jnp.float32)


def kernel(
    feat_hbm, hub_hbm, slot_hbm, nbr_hbm, cnt_hbm, halo_hbm, weight_hbm, bias_hbm,
    out_ref,
    feat, hub, slot, nbr, cnt, halo, weight, bias,
    fhi, flo, halo_rel, one_hot, stage, recv,
    part, part_in, pair_sum, z_in, z_sum, plane_in,
    marks, recip, adjacency, total, w_hi, w_lo,
    in_sem, halo_send, halo_recv, a_sem, b_send, b_recv, c_send, c_recv,
):
    g, l = lax.axis_index("grp"), lax.axis_index("loc")
    y, xh, c = l // 4, (l // 2) % 2, l % 2
    xl, z = g // 4, g % 4
    x = xh * 2 + xl

    def loc_of(dy, dx, dc):
        return ((y + dy) % NY) * 4 + ((xh + dx) % NXH) * 2 + (c + dc) % NC

    def plane_of(dx, dy):
        tx, ty = (x + dx) % 4, (y + dy) % NY
        return (tx % 2) * 4 + z, ty * 4 + (tx // 2) * 2 + c

    loads = []
    for number, (source, target) in enumerate((
        (feat_hbm, feat), (halo_hbm, halo), (hub_hbm, hub), (nbr_hbm, nbr),
        (cnt_hbm, cnt), (weight_hbm, weight), (bias_hbm, bias), (slot_hbm, slot),
    )):
        copy = pltpu.make_async_copy(source, target, in_sem.at[number])
        copy.start()
        loads.append(copy)

    barrier = pltpu.get_barrier_semaphore()
    greeted = 0
    for step in SEND_ORDER:
        if step != (0, 0, 0):
            pl.semaphore_signal(barrier, inc=1, device_id=(g, loc_of(*step)), device_id_type=MESH)
            greeted += 1
    for dz in range(1, NZ):
        pl.semaphore_signal(
            barrier, inc=1, device_id=(xl * 4 + (z + dz) % NZ, l), device_id_type=MESH
        )
        greeted += 1
    for dx in (1, 3):
        for dy in range(NY):
            pl.semaphore_signal(barrier, inc=1, device_id=plane_of(dx, dy), device_id_type=MESH)
            greeted += 1

    loads[1].wait()
    for number, step in enumerate(SEND_ORDER):
        halo_rel[number : number + 1, :] = halo[pl.ds(loc_of(*step), 1), :]
    columns = halo_rel[...].T
    loads[0].wait()
    for start in range(0, ROWS, 256):
        high, low = split2(feat[start : start + 256, :])
        fhi[start : start + 256, :] = high
        flo[start : start + 256, :] = low
    lane = lax.broadcasted_iota(jnp.int32, (SENT, ROWS), 1)
    halo_copies = {}
    for group in range(4):
        for inner in range(4):
            number = group * 4 + inner
            one_hot[inner * SENT : (inner + 1) * SENT, :] = jnp.where(
                lane == columns[:, number : number + 1], 1.0, 0.0
            ).astype(jnp.bfloat16)
        rows = mm(one_hot[...], fhi[...]) + mm(one_hot[...], flo[...])
        for inner in range(4):
            number = group * 4 + inner
            step = SEND_ORDER[number]
            block = rows[inner * SENT : (inner + 1) * SENT, :]
            place = step[0] * NXH + step[1]
            if step == (0, 0, 0):
                recv[place, pl.ds(c, 1)] = block[None]
            else:
                stage[number] = block
        if group == 0:
            pl.semaphore_wait(barrier, greeted)
        for inner in range(4):
            number = group * 4 + inner
            step = SEND_ORDER[number]
            if step != (0, 0, 0):
                copy = pltpu.make_async_remote_copy(
                    src_ref=stage.at[number],
                    dst_ref=recv.at[step[0] * NXH + step[1], c],
                    send_sem=halo_send.at[number],
                    recv_sem=halo_recv.at[number],
                    device_id=(g, loc_of(*step)),
                    device_id_type=MESH,
                )
                copy.start()
                halo_copies[step] = copy

    loads[2].wait()
    upper = lax.broadcasted_iota(jnp.int32, (128, 128), 0) % 8 < 4
    for start in range(0, HUBS, 128):
        rows = mm(hub[start : start + 128, :], fhi[...])
        left, right = rows[:, :128], rows[:, 128:]
        part[0, start : start + 128, :] = jnp.where(upper, left, pltpu.roll(right, 4, 0))
        part[1, start : start + 128, :] = jnp.where(upper, pltpu.roll(left, 124, 0), right)
    pair_copy = pltpu.make_async_remote_copy(
        src_ref=part.at[1 - c],
        dst_ref=part_in,
        send_sem=a_sem.at[0],
        recv_sem=a_sem.at[1],
        device_id=(g, loc_of(0, 0, 1)),
        device_id_type=MESH,
    )
    pair_copy.start()

    loads[3].wait()
    loads[4].wait()
    slots, used = nbr[...], cnt[...]
    active = lax.broadcasted_iota(jnp.int32, (SLOTS, ROWS), 0) < used
    place = slots & (FIELD_ROWS - 1)
    one = jnp.where(active, jnp.left_shift(1, (slots >> 9) * FIELD_BITS), 0)
    inverse = jnp.broadcast_to(1.0 / used.astype(jnp.float32), (8, ROWS))
    for start in range(0, ROWS, 128):
        rows = slice(start, start + 128)
        marks[0, rows, :] = place[:, rows].T
        marks[1, rows, :] = one[:, rows].T
        recip[rows, :] = inverse[:, rows].T

    pool_lane = lax.broadcasted_iota(jnp.int32, (32, FIELD_ROWS), 1)

    def build(block, carry):
        rows = pl.ds(pl.multiple_of(block * 32, 32), 32)
        row_place, row_one = marks[0, rows, :], marks[1, rows, :]
        packed = jnp.zeros((32, FIELD_ROWS), jnp.int32)
        for k in range(SLOTS):
            packed = packed + jnp.where(
                row_place[:, k : k + 1] == pool_lane, row_one[:, k : k + 1], 0
            )
        for field in range(FIELDS):
            number = (packed >> (field * FIELD_BITS)) & (2**FIELD_BITS - 1)
            number = number.astype(jnp.float32).astype(jnp.bfloat16)
            adjacency[2 * field, rows, :] = number[:, :CHUNK]
            adjacency[2 * field + 1, rows, :] = number[:, CHUNK:]
        return carry

    lax.fori_loop(0, 8, build, 0)

    pair_copy.wait_recv()
    own = pl.ds(c, 1)
    pair_sum[...] = (part[own][0] + part_in[...]).reshape(NXL, NZ, 64, 128)
    z_copies = []
    for dz in range(1, NZ):
        to = (z + dz) % NZ
        copy = pltpu.make_async_remote_copy(
            src_ref=pair_sum.at[:, to],
            dst_ref=z_in.at[dz - 1],
            send_sem=b_send.at[dz - 1],
            recv_sem=b_recv.at[dz - 1],
            device_id=(xl * 4 + to, l),
            device_id_type=MESH,
        )
        copy.start()
        z_copies.append(copy)

    lax.fori_loop(8, 24, build, 0)

    for copy in z_copies:
        copy.wait_recv()
    for half in range(NXL):
        value = pair_sum[half, pl.ds(z, 1)][0]
        for dz in range(NZ - 1):
            value = value + z_in[dz, half]
        z_sum[half] = value.reshape(8, 8, 128)
    plane_copies = []
    for dx in range(4):
        for dy in range(NY):
            if (dx, dy) == (0, 0):
                continue
            tx, ty = (x + dx) % 4, (y + dy) % NY
            copy = pltpu.make_async_remote_copy(
                src_ref=z_sum.at[tx % 2, ty * 2 + tx // 2],
                dst_ref=plane_in.at[dx * 4 + dy],
                send_sem=c_send.at[dx * 4 + dy],
                recv_sem=c_recv.at[dx * 4 + dy],
                device_id=plane_of(dx, dy),
                device_id_type=MESH,
            )
            copy.start()
            plane_copies.append(copy)

    lax.fori_loop(24, 32, build, 0)

    for number in range(4):
        rows = slice(number * CHUNK, (number + 1) * CHUNK)
        value = mm(adjacency[number], fhi[rows, :]) + mm(adjacency[number], flo[rows, :])
        total[...] = value if number == 0 else total[...] + value

    loads[5].wait()
    loads[6].wait()
    loads[7].wait()
    w_hi[...], w_lo[...] = split2(weight[...])

    for number, (dy, dx) in enumerate(TAKE_ORDER):
        for dc in range(NC):
            if (dy, dx, dc) != (0, 0, 0):
                halo_copies[(dy, dx, dc)].wait_recv()
        chip = ((y + NY - dy) % NY) * 2 + (xh + NXH - dx) % NXH
        high, low = split2(recv[dy * NXH + dx].reshape(CHUNK, WIDTH))
        links = adjacency[pl.ds(4 + chip, 1)][0]
        total[...] += mm(links, high) + mm(links, low)

    for copy in plane_copies:
        copy.wait_recv()
    hub_tile = z_sum[pl.ds(xl, 1), pl.ds(y * 2 + xh, 1)][0, 0]
    for number in range(1, 16):
        hub_tile = hub_tile + plane_in[number]
    for start in range(0, ROWS, 256):
        rows = slice(start, start + 256)
        index = lax.broadcasted_iota(jnp.int32, (256, WIDTH), 0) + start
        hub_add = jnp.zeros((256, WIDTH), jnp.float32)
        for r in range(HUB_OWN):
            row = jnp.concatenate([hub_tile[r : r + 1, :], hub_tile[4 + r : 5 + r, :]], axis=1)
            hub_add = jnp.where(index == slot[r], row, hub_add)
        combined = feat[rows, :] + total[rows, :] * recip[rows, 0:1] + hub_add
        high, low = split2(combined)
        value = mm(high, w_hi[...]) + mm(low, w_hi[...]) + mm(high, w_lo[...]) + bias[...]
        out_ref[rows, :] = jnp.maximum(value, 0.0)

    for copy in halo_copies.values():
        copy.wait_send()
    pair_copy.wait_send()
    for copy in z_copies + plane_copies:
        copy.wait_send()


def on_device(features, hub_block, hub_slot, neighbours, counts, halo_send, weight, bias):
    f32, bf16, i32 = jnp.float32, jnp.bfloat16, jnp.int32
    vmem, dma = pltpu.VMEM, pltpu.SemaphoreType.DMA
    return pl.pallas_call(
        kernel,
        out_shape=jax.ShapeDtypeStruct((ROWS, WIDTH), f32),
        in_specs=[pl.BlockSpec(memory_space=pltpu.HBM)] * 8,
        out_specs=pl.BlockSpec(memory_space=pltpu.VMEM),
        scratch_shapes=[
            vmem((ROWS, WIDTH), f32),
            vmem((HUBS, ROWS), bf16),
            pltpu.SMEM((HUB_OWN,), i32),
            vmem((SLOTS, ROWS), i32),
            vmem((1, ROWS), i32),
            vmem((16, SENT), i32),
            vmem((WIDTH, WIDTH), f32),
            vmem((1, WIDTH), f32),
            vmem((ROWS, WIDTH), bf16),
            vmem((ROWS, WIDTH), bf16),
            vmem((16, SENT), i32),
            vmem((4 * SENT, ROWS), bf16),
            vmem((16, SENT, WIDTH), f32),
            vmem((8, NC, SENT, WIDTH), f32),
            vmem((NC, HUBS, 128), f32),
            vmem((HUBS, 128), f32),
            vmem((NXL, NZ, 64, 128), f32),
            vmem((NZ - 1, NXL, 64, 128), f32),
            vmem((NXL, 8, 8, 128), f32),
            vmem((16, 8, 128), f32),
            vmem((2, ROWS, SLOTS), i32),
            vmem((ROWS, 8), f32),
            vmem((2 * FIELDS, ROWS, CHUNK), bf16),
            vmem((ROWS, WIDTH), f32),
            vmem((WIDTH, WIDTH), bf16),
            vmem((WIDTH, WIDTH), bf16),
            dma((8,)), dma((16,)), dma((16,)), dma((2,)),
            dma((3,)), dma((3,)), dma((16,)), dma((16,)),
        ],
        compiler_params=pltpu.CompilerParams(
            collective_id=0, has_side_effects=True, vmem_limit_bytes=40 * 1024 * 1024
        ),
    )(
        *(
            pltpu.with_memory_space_constraint(array, pltpu.HBM)
            for array in (
                features, hub_block, hub_slot, neighbours.T, counts.reshape(1, -1), halo_send,
                weight, bias.reshape(1, -1),
            )
        )
    )


def solution(mesh):
    in_specs = (
        P(("grp", "loc"), None),
        P(None, ("grp", "loc")),
        P(("grp", "loc")),
        P(("grp", "loc"), None),
        P(("grp", "loc")),
        P(("grp", "loc"), None),
        P(),
        P(),
    )
    out_specs = P(("grp", "loc"), None)
    return jax.shard_map(
        on_device, mesh=mesh, in_specs=in_specs, out_specs=out_specs, check_vma=False
    )
```

```python
import jax
import jax.numpy as jnp
from jax import lax
from jax.experimental import pallas as pl
from jax.experimental.pallas import tpu as pltpu
from jax.sharding import PartitionSpec as P

MESH = pl.DeviceIdType.MESH
NY, NXH, NC, NXL, NZ = 4, 2, 2, 2, 4
ROWS, WIDTH, SLOTS, SENT = 1024, 256, 16, 128
HUBS, HUB_OWN = 512, 4
FIELD_ROWS, FIELDS, FIELD_BITS = 512, 6, 5

SEND_ORDER = (
    (2, 1, 0), (1, 0, 0), (2, 1, 1), (3, 0, 0),
    (1, 1, 0), (1, 1, 1), (2, 0, 0), (0, 0, 1),
    (3, 1, 0), (3, 1, 1), (2, 0, 1), (0, 0, 0),
    (0, 1, 0), (0, 1, 1), (1, 0, 1), (3, 0, 1),
)
GROUPS = (2, 2, 4, 4, 4)
TAKE_ORDER = (
    (0, 0, 0), (0, 0, 1), (2, 1, 0), (1, 0, 0), (3, 0, 0), (2, 1, 1), (1, 1, 0), (1, 1, 1),
    (2, 0, 0), (3, 1, 0), (3, 1, 1), (2, 0, 1), (1, 0, 1), (3, 0, 1), (0, 1, 0), (0, 1, 1),
)

def split2(value):
    high = value.astype(jnp.bfloat16)
    low = (value - high.astype(jnp.float32)).astype(jnp.bfloat16)
    return high, low


def mm(left, right):
    return jnp.dot(left, right, preferred_element_type=jnp.float32)


def scope(name):
    return jax.named_scope(name)


def kernel(
    feat_hbm, hub_hbm, slot_hbm, nbr_hbm, cnt_hbm, halo_hbm, weight_hbm, bias_hbm,
    out_ref,
    feat, hub, slot, nbr, cnt, halo, weight, bias,
    fhi, base, ghi, glo, halo_rel, one_hot, stage, recv,
    part, part_in, pair_sum, z_in, z_sum, plane_in,
    marks, recip, hub_mark, links_own, links_far, total, w_hi, w_lo,
    in_sem, halo_send, halo_recv, a_sem, b_send, b_recv, c_send, c_recv,
):
    g, l = lax.axis_index("grp"), lax.axis_index("loc")
    y, xh, c = l // 4, (l // 2) % 2, l % 2
    xl, z = g // 4, g % 4
    x = xh * 2 + xl

    def loc_of(dy, dx, dc):
        return ((y + dy) % NY) * 4 + ((xh + dx) % NXH) * 2 + (c + dc) % NC

    def plane_of(dx, dy):
        tx, ty = (x + dx) % 4, (y + dy) % NY
        return (tx % 2) * 4 + z, ty * 4 + (tx // 2) * 2 + c

    loads = []
    for number, (source, target) in enumerate((
        (feat_hbm, feat), (halo_hbm, halo), (weight_hbm, weight), (hub_hbm, hub), (nbr_hbm, nbr),
        (cnt_hbm, cnt), (bias_hbm, bias), (slot_hbm, slot),
    )):
        copy = pltpu.make_async_copy(source, target, in_sem.at[number])
        copy.start()
        loads.append(copy)

    with scope("greet"):
        barrier = pltpu.get_barrier_semaphore()
        greeted = 0
        for dx, dy in ((1, 2), (3, 2), (1, 1), (1, 3), (3, 1), (3, 3), (1, 0), (3, 0)):
            pl.semaphore_signal(barrier, inc=1, device_id=plane_of(dx, dy), device_id_type=MESH)
            greeted += 1
        for step in SEND_ORDER:
            if step != (0, 0, 0):
                pl.semaphore_signal(
                    barrier, inc=1, device_id=(g, loc_of(*step)), device_id_type=MESH
                )
                greeted += 1
        for dz in range(1, NZ):
            pl.semaphore_signal(
                barrier, inc=1, device_id=(xl * 4 + (z + dz) % NZ, l), device_id_type=MESH
            )
            greeted += 1

    with scope("halo_idx"):
        loads[1].wait()
        for number, step in enumerate(SEND_ORDER):
            halo_rel[number : number + 1, :] = halo[pl.ds(loc_of(*step), 1), :]
        columns = halo_rel[...].T
        loads[2].wait()
        w_hi[...], w_lo[...] = split2(weight[...])
        loads[0].wait()
    with scope("fw"):
        for start in range(0, ROWS, 256):
            rows = slice(start, start + 256)
            high, low = split2(feat[rows, :])
            fhi[rows, :] = high
            value = mm(high, w_hi[...]) + mm(low, w_hi[...]) + mm(high, w_lo[...])
            base[rows, :] = value
            ghi[rows, :], glo[rows, :] = split2(value)

    lane = lax.broadcasted_iota(jnp.int32, (SENT, ROWS), 1)
    halo_copies = {}

    def gather(group):
        first, size = sum(GROUPS[:group]), GROUPS[group]
        with scope(f"oh{group}"):
            for inner in range(size):
                number = first + inner
                one_hot[inner * SENT : (inner + 1) * SENT, :] = jnp.where(
                    lane == columns[:, number : number + 1], 1.0, 0.0
                ).astype(jnp.bfloat16)
        with scope(f"gmm{group}"):
            hot = one_hot[: size * SENT, :]
            rows = mm(hot, ghi[...]) + mm(hot, glo[...])
            for inner in range(size):
                number = first + inner
                block = rows[inner * SENT : (inner + 1) * SENT, :]
                if SEND_ORDER[number] == (0, 0, 0):
                    recv[number] = block
                else:
                    stage[number] = block

    def send(group):
        first, size = sum(GROUPS[:group]), GROUPS[group]
        for number in range(first, first + size):
            step = SEND_ORDER[number]
            if step != (0, 0, 0):
                copy = pltpu.make_async_remote_copy(
                    src_ref=stage.at[number],
                    dst_ref=recv.at[number],
                    send_sem=halo_send.at[number],
                    recv_sem=halo_recv.at[number],
                    device_id=(g, loc_of(*step)),
                    device_id_type=MESH,
                )
                copy.start()
                halo_copies[step] = copy

    gather(0)
    with scope("barrier"):
        pl.semaphore_wait(barrier, greeted)
    send(0)
    gather(1)
    send(1)

    with scope("hubpart"):
        loads[3].wait()
        upper = lax.broadcasted_iota(jnp.int32, (128, 128), 0) % 8 < 4
        for start in range(0, HUBS, 128):
            rows = mm(hub[start : start + 128, :], fhi[...])
            left, right = rows[:, :128], rows[:, 128:]
            part[0, start : start + 128, :] = jnp.where(upper, left, pltpu.roll(right, 4, 0))
            part[1, start : start + 128, :] = jnp.where(upper, pltpu.roll(left, 124, 0), right)
        pair_copy = pltpu.make_async_remote_copy(
            src_ref=part.at[1 - c],
            dst_ref=part_in,
            send_sem=a_sem.at[0],
            recv_sem=a_sem.at[1],
            device_id=(g, loc_of(0, 0, 1)),
            device_id_type=MESH,
        )
        pair_copy.start()

    gather(2)
    send(2)
    with scope("a_to_b"):
        pair_copy.wait_recv()
        pair_sum[...] = (part[pl.ds(c, 1)][0] + part_in[...]).reshape(NXL, NZ, 64, 128)
        z_copies = []
        for dz in range(1, NZ):
            to = (z + dz) % NZ
            copy = pltpu.make_async_remote_copy(
                src_ref=pair_sum.at[:, to],
                dst_ref=z_in.at[dz - 1],
                send_sem=b_send.at[dz - 1],
                recv_sem=b_recv.at[dz - 1],
                device_id=(xl * 4 + to, l),
                device_id_type=MESH,
            )
            copy.start()
            z_copies.append(copy)

    gather(3)
    gather(4)

    with scope("marks"):
        loads[4].wait()
        loads[5].wait()
        slots, used = nbr[...], cnt[...]
        active = lax.broadcasted_iota(jnp.int32, (SLOTS, ROWS), 0) < used
        place = slots & (FIELD_ROWS - 1)
        one = jnp.where(active, jnp.left_shift(1, (slots >> 9) * FIELD_BITS), 0)
        inverse = jnp.broadcast_to(1.0 / used.astype(jnp.float32), (8, ROWS))
        for start in range(0, ROWS, 128):
            rows = slice(start, start + 128)
            marks[0, rows, :] = place[:, rows].T
            marks[1, rows, :] = one[:, rows].T
            recip[rows, :] = inverse[:, rows].T

    pool_lane = lax.broadcasted_iota(jnp.int32, (32, FIELD_ROWS), 1)

    def build(block, carry):
        rows = pl.ds(pl.multiple_of(block * 32, 32), 32)
        row_place, row_one = marks[0, rows, :], marks[1, rows, :]
        packed = jnp.zeros((32, FIELD_ROWS), jnp.int32)
        for k in range(SLOTS):
            packed = packed + jnp.where(
                row_place[:, k : k + 1] == pool_lane, row_one[:, k : k + 1], 0
            )
        for field in range(FIELDS):
            number = (packed >> (field * FIELD_BITS)) & (2**FIELD_BITS - 1)
            number = number.astype(jnp.float32).astype(jnp.bfloat16)
            if field < 2:
                links_own[2 * field, rows, :] = number[:, :256]
                links_own[2 * field + 1, rows, :] = number[:, 256:]
            else:
                for peer in range(4):
                    links_far[(field - 2) * 4 + peer, rows, :] = number[
                        :, peer * SENT : (peer + 1) * SENT
                    ]
        return carry

    with scope("build1"):
        lax.fori_loop(0, 8, build, 0)

    with scope("b_to_c"):
        for copy in z_copies:
            copy.wait_recv()
        for half in range(NXL):
            value = pair_sum[half, pl.ds(z, 1)][0]
            for dz in range(NZ - 1):
                value = value + z_in[dz, half]
            z_sum[half] = value.reshape(8, 8, 128)
        plane_copies = []
        for dx in range(4):
            for dy in range(NY):
                if (dx, dy) == (0, 0):
                    continue
                tx, ty = (x + dx) % 4, (y + dy) % NY
                copy = pltpu.make_async_remote_copy(
                    src_ref=z_sum.at[tx % 2, ty * 2 + tx // 2],
                    dst_ref=plane_in.at[dx * 4 + dy],
                    send_sem=c_send.at[dx * 4 + dy],
                    recv_sem=c_recv.at[dx * 4 + dy],
                    device_id=plane_of(dx, dy),
                    device_id_type=MESH,
                )
                copy.start()
                plane_copies.append(copy)

    send(3)
    send(4)

    with scope("build3"):
        lax.fori_loop(8, 32, build, 0)

    with scope("hub_mark"):
        loads[6].wait()
        loads[7].wait()
        for r in range(HUB_OWN):
            hit = lax.broadcasted_iota(jnp.int32, (ROWS, WIDTH), 0) == slot[r]
            hub_mark[r] = jnp.where(hit, 1.0, 0.0)
        base[...] = base[...] + bias[...]

    with scope("own"):
        for number in range(4):
            rows = slice(number * 256, (number + 1) * 256)
            value = mm(links_own[number], ghi[rows, :]) + mm(links_own[number], glo[rows, :])
            total[...] = value if number == 0 else total[...] + value

    def far(step):
        number = SEND_ORDER.index(step)
        dy, dx, dc = step
        if step != (0, 0, 0):
            with scope(f"wait{dy}{dx}{dc}"):
                halo_copies[step].wait_recv()
        peer = loc_of(-dy, -dx, -dc)
        high, low = split2(recv[number])
        return peer, jnp.concatenate([high, low], axis=0)

    def linked(peer, rows):
        links = links_far[pl.ds(peer, 1), rows, :][0]
        return jnp.concatenate([links, links], axis=1)

    for number, step in enumerate(TAKE_ORDER[:-1]):
        peer, values = far(step)
        with scope(f"take{number}"):
            total[...] += mm(linked(peer, slice(None)), values)

    peer, values = far(TAKE_ORDER[-1])
    with scope("wait_c"):
        for copy in plane_copies:
            copy.wait_recv()
    with scope("hub_rows"):
        hub_tile = z_sum[pl.ds(xl, 1), pl.ds(y * 2 + xh, 1)][0, 0]
        for source in range(1, 16):
            hub_tile = hub_tile + plane_in[source]
        hub_own = jnp.concatenate([hub_tile, pltpu.roll(hub_tile, 4, 0)], axis=1)
        high, low = split2(hub_own)
        hub_own = mm(high, w_hi[...]) + mm(low, w_hi[...]) + mm(high, w_lo[...])
    with scope("final"):
        for start in range(0, ROWS, 256):
            rows = slice(start, start + 256)
            value = total[rows, :] + mm(linked(peer, rows), values)
            value = base[rows, :] + value * recip[rows, 0:1]
            for r in range(HUB_OWN):
                value = value + hub_mark[r, rows, :] * hub_own[r : r + 1, :]
            out_ref[rows, :] = jnp.maximum(value, 0.0)

    with scope("wait_send"):
        for copy in halo_copies.values():
            copy.wait_send()
        pair_copy.wait_send()
        for copy in z_copies + plane_copies:
            copy.wait_send()


def on_device(features, hub_block, hub_slot, neighbours, counts, halo_send, weight, bias):
    f32, bf16, i32 = jnp.float32, jnp.bfloat16, jnp.int32
    vmem, dma = pltpu.VMEM, pltpu.SemaphoreType.DMA
    return pl.pallas_call(
        kernel,
        out_shape=jax.ShapeDtypeStruct((ROWS, WIDTH), f32),
        in_specs=[pl.BlockSpec(memory_space=pltpu.HBM)] * 8,
        out_specs=pl.BlockSpec(memory_space=pltpu.VMEM),
        scratch_shapes=[
            vmem((ROWS, WIDTH), f32),
            vmem((HUBS, ROWS), bf16),
            pltpu.SMEM((HUB_OWN,), i32),
            vmem((SLOTS, ROWS), i32),
            vmem((1, ROWS), i32),
            vmem((16, SENT), i32),
            vmem((WIDTH, WIDTH), f32),
            vmem((1, WIDTH), f32),
            vmem((ROWS, WIDTH), bf16),
            vmem((ROWS, WIDTH), f32),
            vmem((ROWS, WIDTH), bf16),
            vmem((ROWS, WIDTH), bf16),
            vmem((16, SENT), i32),
            vmem((4 * SENT, ROWS), bf16),
            vmem((16, SENT, WIDTH), f32),
            vmem((16, SENT, WIDTH), f32),
            vmem((NC, HUBS, 128), f32),
            vmem((HUBS, 128), f32),
            vmem((NXL, NZ, 64, 128), f32),
            vmem((NZ - 1, NXL, 64, 128), f32),
            vmem((NXL, 8, 8, 128), f32),
            vmem((16, 8, 128), f32),
            vmem((2, ROWS, SLOTS), i32),
            vmem((ROWS, 8), f32),
            vmem((HUB_OWN, ROWS, WIDTH), f32),
            vmem((4, ROWS, 256), bf16),
            vmem((16, ROWS, SENT), bf16),
            vmem((ROWS, WIDTH), f32),
            vmem((WIDTH, WIDTH), bf16),
            vmem((WIDTH, WIDTH), bf16),
            dma((8,)), dma((16,)), dma((16,)), dma((2,)),
            dma((3,)), dma((3,)), dma((16,)), dma((16,)),
        ],
        compiler_params=pltpu.CompilerParams(
            collective_id=0, has_side_effects=True, vmem_limit_bytes=40 * 1024 * 1024
        ),
    )(
        *(
            pltpu.with_memory_space_constraint(array, pltpu.HBM)
            for array in (
                features, hub_block, hub_slot, neighbours.T, counts.reshape(1, -1), halo_send,
                weight, bias.reshape(1, -1),
            )
        )
    )


def solution(mesh):
    in_specs = (
        P(("grp", "loc"), None),
        P(None, ("grp", "loc")),
        P(("grp", "loc")),
        P(("grp", "loc"), None),
        P(("grp", "loc")),
        P(("grp", "loc"), None),
        P(),
        P(),
    )
    out_specs = P(("grp", "loc"), None)
    return jax.shard_map(
        on_device, mesh=mesh, in_specs=in_specs, out_specs=out_specs, check_vma=False
    )
```

```python
import jax
import jax.numpy as jnp
from jax import lax
from jax.experimental import pallas as pl
from jax.experimental.pallas import tpu as pltpu
from jax.sharding import PartitionSpec as P

MESH = pl.DeviceIdType.MESH
NY, NXH, NC, NXL, NZ = 4, 2, 2, 2, 4
ROWS, WIDTH, SLOTS, SENT = 1024, 256, 16, 128
HUBS, HUB_OWN = 512, 4
FIELD_ROWS, FIELDS, FIELD_BITS = 512, 6, 5

PLAN = (
    (((2, 1, 0), ), ()),
    (((1, 0, 0), (2, 1, 1), (3, 0, 0), ), ()),
    (((1, 1, 0), (2, 0, 0), (3, 1, 0), (2, 0, 1), (1, 0, 1), (3, 0, 1), (0, 0, 1), (0, 0, 0), ), ()),
    (((1, 1, 1), (3, 1, 1), ), ()),
    ((), ((2, 1, 0), )),
    ((), ((2, 1, 1), )),
    ((), ()),
    (((0, 1, 0), (0, 1, 1), ), ()),
    ((), ((1, 1, 0), )),
)
TAKE_ORDER = (
    ("take", (0, 0, 0)), ("take", (0, 0, 1)), ("forward", (3, 1, 0)),
    ("take", (1, 0, 0)), ("take", (3, 0, 0)), ("take", (2, 0, 0)),
    ("forward", (1, 1, 1)), ("take", (2, 0, 1)), ("take", (1, 0, 1)),
    ("take", (3, 0, 1)), ("take", (2, 1, 0)), ("forward", (3, 1, 1)),
    ("take", (2, 1, 1)), ("take", (1, 1, 0)), ("hub", (0, 0, 0)),
    ("take", (0, 1, 0)), ("take", (3, 1, 0)), ("last", (1, 1, 1)),
    ("last", (3, 1, 1)), ("last", (0, 1, 1)),
)


ORDER = tuple(step for sends, _ in PLAN for step in sends)
RELAYED = tuple(step for step in ORDER if step[0] != 0 and step[1] != 0)


def split2(value):
    high = value.astype(jnp.bfloat16)
    low = (value - high.astype(jnp.float32)).astype(jnp.bfloat16)
    return high, low


def mm(left, right):
    return jnp.dot(left, right, preferred_element_type=jnp.float32)


def scope(name):
    return jax.named_scope(name)


def kernel(
    feat_hbm, hub_hbm, slot_hbm, nbr_hbm, cnt_hbm, halo_hbm, weight_hbm, bias_hbm,
    out_ref,
    feat, hub, slot, nbr, cnt, halo, weight, bias,
    fhi, base, table, ghi, glo, stage, recv, relay,
    part, part_in, pair_sum, z_in, z_sum, plane_in,
    marks, recip, hub_mark, links_own, links_far, total, w_hi, w_lo,
    in_sem, halo_send, halo_recv, relay_send, relay_recv, a_sem, b_send, b_recv, c_send, c_recv, others_in,
):
    g, l = lax.axis_index("grp"), lax.axis_index("loc")
    y, xh, c = l // 4, (l // 2) % 2, l % 2
    xl, z = g // 4, g % 4
    x = xh * 2 + xl

    def loc_of(dy, dx, dc):
        return ((y + dy + 2 * c * dy) % NY) * 4 + ((xh + dx) % NXH) * 2 + (c + dc) % NC

    def loc_from(dy, dx, dc):
        source = (c + dc) % NC
        return ((y - dy - 2 * source * dy + 3 * NY) % NY) * 4 + ((xh + dx) % NXH) * 2 + source

    def plane_of(dx, dy):
        tx, ty = (x + dx) % 4, (y + dy) % NY
        return (tx % 2) * 4 + z, ty * 4 + (tx // 2) * 2 + c

    quarter = [pl.ds(start, 256) for start in range(0, ROWS, 256)]
    loads = []
    for number, (source, target) in enumerate((
        *((feat_hbm.at[q], feat.at[q]) for q in quarter), (weight_hbm, weight), (halo_hbm, halo),
        (hub_hbm, hub), (nbr_hbm, nbr), (cnt_hbm, cnt), (bias_hbm, bias), (slot_hbm, slot),
    )):
        copy = pltpu.make_async_copy(source, target, in_sem.at[number])
        copy.start()
        loads.append(copy)

    def signal(semaphore, where):
        pl.semaphore_signal(semaphore, inc=1, device_id=where, device_id_type=MESH)

    barrier = pltpu.get_barrier_semaphore()
    beside = (plane_of(1, 0), plane_of(3, 0))
    greeted = [(g, loc_of(*step)) for step in ORDER if step != (0, 0, 0)]
    greeted += beside
    for where in greeted:
        signal(barrier, where)
    ring = [(z + dz) % NZ for dz in range(1, NZ)]
    for to in ring:

        @pl.when((z != 0) & (to != 0))
        def _():
            signal(barrier, (xl * 4 + to, l))

    with scope("inputs"):
        loads[4].wait()
        w_hi[...], w_lo[...] = split2(weight[...])
        for copy in loads[:4]:
            copy.wait()

    def weighed(value):
        high, low = split2(value)
        return high, mm(high, w_hi[...]) + mm(low, w_hi[...]) + mm(high, w_lo[...])

    with scope("fw"):
        for start in range(0, ROWS, 256):
            rows = slice(start, start + 256)
            fhi[rows, :], value = weighed(feat[rows, :])
            for half in range(2):
                table[rows, half, :] = value[:, half * 128 : (half + 1) * 128]
        loads[5].wait()

    halo_copies, relay_copies, sent = {}, {}, []

    def gather(number):
        step = ORDER[number]
        peer = loc_of(*step)
        target = recv if step == (0, 0, 0) else stage
        for row in range(SENT):
            target[number, row] = table[halo[peer, row]]

    def start_copy(source, target, send_sem, recv_sem, where):
        copy = pltpu.make_async_remote_copy(
            src_ref=source, dst_ref=target, send_sem=send_sem, recv_sem=recv_sem,
            device_id=(g, where), device_id_type=MESH,
        )
        copy.start()
        sent.append(copy)
        return copy

    def send(step):
        number = ORDER.index(step)
        if step in RELAYED:
            at = RELAYED.index(step)
            relay_copies[step] = start_copy(
                stage.at[number], relay.at[at], halo_send.at[number], relay_recv.at[at],
                loc_of(0, 1, 0),
            )
        elif step != (0, 0, 0):
            halo_copies[step] = start_copy(
                stage.at[number], recv.at[number], halo_send.at[number], halo_recv.at[number],
                loc_of(*step),
            )

    def forward(step):
        number, at = ORDER.index(step), RELAYED.index(step)
        with scope(f"relay{step[0]}{step[2]}"):
            relay_copies[step].wait_recv()
        halo_copies[step] = start_copy(
            relay.at[at], recv.at[number], relay_send.at[at], halo_recv.at[number],
            loc_of(step[0], 0, step[2]),
        )

    def exchange(stage_number):
        for step in PLAN[stage_number][0]:
            if stage_number < 3 and step != ORDER[0]:
                gather(ORDER.index(step))
            send(step)
        for step in PLAN[stage_number][1]:
            forward(step)

    with scope("gather0"):
        gather(0)
    with scope("barrier"):
        pl.semaphore_wait(barrier, len(greeted) + jnp.where(z == 0, 0, NZ - 1))
    exchange(0)

    for to in ring:

        @pl.when((z == 0) | (to == 0))
        def _():
            signal(barrier, (xl * 4 + to, l))

    for number, where in enumerate(beside):
        signal(others_in.at[number], where)

    with scope("gather1"):
        exchange(1)

    with scope("hubpart"):
        loads[6].wait()
        upper = lax.broadcasted_iota(jnp.int32, (128, 128), 0) % 8 < 4
        for start in range(0, HUBS, 128):
            rows = mm(hub[start : start + 128, :], fhi[...])
            left, right = rows[:, :128], rows[:, 128:]
            part[0, start : start + 128, :] = jnp.where(upper, left, pltpu.roll(right, 4, 0))
            part[1, start : start + 128, :] = jnp.where(upper, pltpu.roll(left, 124, 0), right)
        pair_copy = pltpu.make_async_remote_copy(
            src_ref=part.at[1 - c],
            dst_ref=part_in,
            send_sem=a_sem.at[0],
            recv_sem=a_sem.at[1],
            device_id=(g, loc_of(0, 0, 1)),
            device_id_type=MESH,
        )
        pair_copy.start()

    with scope("gather2"):
        exchange(2)
        for number in range(sum(len(sends) for sends, _ in PLAN[:3]), len(ORDER)):
            gather(number)

    with scope("a_to_b"):
        pair_copy.wait_recv()
        pair_sum[...] = (part[pl.ds(c, 1)][0] + part_in[...]).reshape(NXL, NZ, 64, 128)
        z_copies = []

        @pl.when(z == 0)
        def _():
            pl.semaphore_wait(barrier, NZ - 1)

        for dz in range(1, NZ):
            to = (z + dz) % NZ
            copy = pltpu.make_async_remote_copy(
                src_ref=pair_sum.at[:, to],
                dst_ref=z_in.at[dz - 1],
                send_sem=b_send.at[dz - 1],
                recv_sem=b_recv.at[dz - 1],
                device_id=(xl * 4 + to, l),
                device_id_type=MESH,
            )
            copy.start()
            z_copies.append(copy)


    with scope("marks"):
        loads[7].wait()
        loads[8].wait()
        slots, used = nbr[...], cnt[...]
        active = lax.broadcasted_iota(jnp.int32, (SLOTS, ROWS), 0) < used
        place = slots & (FIELD_ROWS - 1)
        one = jnp.where(active, jnp.left_shift(1, (slots >> 9) * FIELD_BITS), 0)
        inverse = jnp.broadcast_to(1.0 / used.astype(jnp.float32), (8, ROWS))
        for start in range(0, ROWS, 128):
            rows = slice(start, start + 128)
            marks[0, rows, :] = place[:, rows].T
            marks[1, rows, :] = one[:, rows].T
            recip[rows, :] = inverse[:, rows].T

    pool_lane = lax.broadcasted_iota(jnp.int32, (32, FIELD_ROWS), 1)

    def build(block, carry):
        rows = pl.ds(pl.multiple_of(block * 32, 32), 32)
        row_place, row_one = marks[0, rows, :], marks[1, rows, :]
        packed = jnp.zeros((32, FIELD_ROWS), jnp.int32)
        for k in range(SLOTS):
            packed = packed + jnp.where(
                row_place[:, k : k + 1] == pool_lane, row_one[:, k : k + 1], 0
            )
        for field in range(FIELDS):
            number = (packed >> (field * FIELD_BITS)) & (2**FIELD_BITS - 1)
            number = number.astype(jnp.float32).astype(jnp.bfloat16)
            if field < 2:
                links_own[2 * field, rows, :] = number[:, :256]
                links_own[2 * field + 1, rows, :] = number[:, 256:]
            else:
                for peer in range(4):
                    links = number[:, peer * SENT : (peer + 1) * SENT]
                    for half in range(2):
                        lanes = slice(half * SENT, (half + 1) * SENT)
                        links_far[(field - 2) * 4 + peer, rows, lanes] = links
        return carry

    exchange(3)
    with scope("build1"):
        lax.fori_loop(0, 8, build, 0)
    exchange(4)
    with scope("build2"):
        lax.fori_loop(8, 16, build, 0)
    exchange(5)
    with scope("build3"):
        lax.fori_loop(16, 24, build, 0)
    exchange(6)
    with scope("b_to_c"):
        for copy in z_copies:
            copy.wait_recv()
        for half in range(NXL):
            value = pair_sum[half, pl.ds(z, 1)][0]
            for dz in range(NZ - 1):
                value = value + z_in[dz, half]
            z_sum[half] = value.reshape(8, 8, 128)
        plane_copies = []
        for number in (0, 1):
            pl.semaphore_wait(others_in.at[number], 1)
        for dx in range(4):
            for dy in range(NY):
                if (dx, dy) == (0, 0):
                    continue
                tx, ty = (x + dx) % 4, (y + dy) % NY
                copy = pltpu.make_async_remote_copy(
                    src_ref=z_sum.at[tx % 2, ty * 2 + tx // 2],
                    dst_ref=plane_in.at[dx * 4 + dy],
                    send_sem=c_send.at[dx * 4 + dy],
                    recv_sem=c_recv.at[dx * 4 + dy],
                    device_id=plane_of(dx, dy),
                    device_id_type=MESH,
                )
                copy.start()
                plane_copies.append(copy)

    exchange(7)
    with scope("build4"):
        lax.fori_loop(24, 32, build, 0)
    exchange(8)

    with scope("hub_mark"):
        loads[9].wait()
        loads[10].wait()
        vertex = lax.broadcasted_iota(jnp.int32, (ROWS, 128), 0)
        lane = lax.broadcasted_iota(jnp.int32, (ROWS, 128), 1)
        mark = jnp.zeros((ROWS, 128), jnp.float32)
        for r in range(HUB_OWN):
            mark = jnp.where((vertex == slot[r]) & ((lane == r) | (lane == 4 + r)), 1.0, mark)
        hub_mark[...] = mark.astype(jnp.bfloat16)
        for start in range(0, ROWS, 256):
            rows = slice(start, start + 256)
            halves = [table[rows, half, :] for half in range(2)]
            value = jnp.concatenate(halves, axis=1)
            base[rows, :] = value + bias[...]
            ghi[rows, :], glo[rows, :] = split2(value)

    with scope("own"):
        for number in range(4):
            rows = slice(number * 256, (number + 1) * 256)
            value = mm(links_own[number], ghi[rows, :]) + mm(links_own[number], glo[rows, :])
            total[...] = value if number == 0 else total[...] + value

    def far(step):
        number = ORDER.index(step)
        dy, dx, dc = step
        if step != (0, 0, 0):
            with scope(f"wait{dy}{dx}{dc}"):
                halo_copies[step].wait_recv()
        peer = loc_from(dy, dx, dc)
        halves = [recv[number, :, half, :] for half in range(2)]
        high, low = split2(jnp.concatenate(halves, axis=1))
        return peer, jnp.concatenate([high, low], axis=0)

    def linked(peer, rows):
        return links_far[pl.ds(peer, 1), rows, :][0]

    def hub_rows():
        with scope("wait_c"):
            for copy in plane_copies:
                copy.wait_recv()
        with scope("hub_rows"):
            hub_tile = z_sum[pl.ds(xl, 1), pl.ds(y * 2 + xh, 1)][0, 0]
            for source in range(1, 16):
                hub_tile = hub_tile + plane_in[source]
            hub_own = weighed(jnp.concatenate([hub_tile, pltpu.roll(hub_tile, 4, 0)], axis=1))[1]
            upper = lax.broadcasted_iota(jnp.int32, (8, WIDTH), 0) < HUB_OWN
            high = hub_own.astype(jnp.bfloat16).astype(jnp.float32)
            both = jnp.where(upper, high, pltpu.roll(hub_own - high, 4, 0))
            hub_values = jnp.concatenate([both, jnp.zeros((120, WIDTH), jnp.float32)], axis=0)
            hub_values = hub_values.astype(jnp.bfloat16)
            base[...] += mm(hub_mark[...], hub_values)

    for kind, step in TAKE_ORDER:
        if kind == "hub":
            hub_rows()
        elif kind == "forward":
            forward(step)
        elif kind == "take":
            peer, values = far(step)
            with scope("take"):
                total[...] += mm(linked(peer, slice(None)), values)

    with scope("combine"):
        base[...] += total[...] * recip[:, 0:1]
    last = [far(step) for kind, step in TAKE_ORDER if kind == "last"]
    with scope("final"):
        for start in range(0, ROWS, 256):
            rows = slice(start, start + 256)
            value = sum(mm(linked(peer, rows), values) for peer, values in last)
            out_ref[rows, :] = jnp.maximum(base[rows, :] + value * recip[rows, 0:1], 0.0)

    with scope("wait_send"):
        for copy in sent:
            copy.wait_send()
        pair_copy.wait_send()
        for copy in z_copies + plane_copies:
            copy.wait_send()


def on_device(features, hub_block, hub_slot, neighbours, counts, halo_send, weight, bias):
    f32, bf16, i32 = jnp.float32, jnp.bfloat16, jnp.int32
    vmem, dma = pltpu.VMEM, pltpu.SemaphoreType.DMA
    return pl.pallas_call(
        kernel,
        out_shape=jax.ShapeDtypeStruct((ROWS, WIDTH), f32),
        in_specs=[pl.BlockSpec(memory_space=pltpu.HBM)] * 8,
        out_specs=pl.BlockSpec(memory_space=pltpu.VMEM),
        scratch_shapes=[
            vmem((ROWS, WIDTH), f32),
            vmem((HUBS, ROWS), bf16),
            pltpu.SMEM((HUB_OWN,), i32),
            vmem((SLOTS, ROWS), i32),
            vmem((1, ROWS), i32),
            pltpu.SMEM((16, SENT), i32),
            vmem((WIDTH, WIDTH), f32),
            vmem((1, WIDTH), f32),
            vmem((ROWS, WIDTH), bf16),
            vmem((ROWS, WIDTH), f32),
            vmem((ROWS, 2, 128), f32),
            vmem((ROWS, WIDTH), bf16),
            vmem((ROWS, WIDTH), bf16),
            vmem((16, SENT, 2, 128), f32),
            vmem((16, SENT, 2, 128), f32),
            vmem((6, SENT, 2, 128), f32),
            vmem((NC, HUBS, 128), f32),
            vmem((HUBS, 128), f32),
            vmem((NXL, NZ, 64, 128), f32),
            vmem((NZ - 1, NXL, 64, 128), f32),
            vmem((NXL, 8, 8, 128), f32),
            vmem((16, 8, 128), f32),
            vmem((2, ROWS, SLOTS), i32),
            vmem((ROWS, 8), f32),
            vmem((ROWS, 128), bf16),
            vmem((4, ROWS, 256), bf16),
            vmem((16, ROWS, 2 * SENT), bf16),
            vmem((ROWS, WIDTH), f32),
            vmem((WIDTH, WIDTH), bf16),
            vmem((WIDTH, WIDTH), bf16),
            dma((11,)), dma((16,)), dma((16,)), dma((6,)), dma((6,)), dma((2,)),
            dma((3,)), dma((3,)), dma((16,)), dma((16,)), pltpu.SemaphoreType.REGULAR((2,)),
        ],
        compiler_params=pltpu.CompilerParams(
            collective_id=0, has_side_effects=True, vmem_limit_bytes=40 * 1024 * 1024
        ),
    )(
        *(
            pltpu.with_memory_space_constraint(array, pltpu.HBM)
            for array in (
                features, hub_block, hub_slot, neighbours.T, counts.reshape(1, -1), halo_send,
                weight, bias.reshape(1, -1),
            )
        )
    )


def solution(mesh):
    in_specs = (
        P(("grp", "loc"), None),
        P(None, ("grp", "loc")),
        P(("grp", "loc")),
        P(("grp", "loc"), None),
        P(("grp", "loc")),
        P(("grp", "loc"), None),
        P(),
        P(),
    )
    out_specs = P(("grp", "loc"), None)
    return jax.shard_map(
        on_device, mesh=mesh, in_specs=in_specs, out_specs=out_specs, check_vma=False
    )
```

```python
import jax
import jax.numpy as jnp
from jax import lax
from jax.experimental import pallas as pl
from jax.experimental.pallas import tpu as pltpu
from jax.sharding import PartitionSpec as P

MESH = pl.DeviceIdType.MESH
NY, NXH, NC, NXL, NZ = 4, 2, 2, 2, 4
ROWS, WIDTH, SLOTS, SENT = 1024, 256, 16, 128
HUBS, HUB_OWN = 512, 4
FIELD_ROWS, FIELDS, FIELD_BITS = 512, 6, 5

PLAN = (
    (((2, 1, 0), ), ()),
    (((1, 0, 0), (2, 1, 1), (3, 0, 0), ), ()),
    (((1, 1, 0), (2, 0, 0), (3, 1, 0), (2, 0, 1), (1, 0, 1), (3, 0, 1), (0, 0, 1), (0, 0, 0), ), ()),
    (((1, 1, 1), (3, 1, 1), ), ()),
    ((), ((2, 1, 0), )),
    ((), ((2, 1, 1), )),
    ((), ()),
    (((0, 1, 0), (0, 1, 1), ), ()),
    ((), ((1, 1, 0), )),
)
TAKE_ORDER = (
    ("take", (0, 0, 0)), ("take", (0, 0, 1)), ("forward", (3, 1, 0)),
    ("take", (1, 0, 0)), ("take", (3, 0, 0)), ("take", (2, 0, 0)),
    ("forward", (1, 1, 1)), ("take", (2, 0, 1)), ("take", (1, 0, 1)),
    ("take", (3, 0, 1)), ("take", (2, 1, 0)), ("forward", (3, 1, 1)),
    ("take", (2, 1, 1)), ("take", (1, 1, 0)), ("hub", (0, 0, 0)),
    ("take", (0, 1, 0)), ("take", (3, 1, 0)), ("last", (1, 1, 1)),
    ("last", (3, 1, 1)), ("last", (0, 1, 1)),
)


ORDER = tuple(step for sends, _ in PLAN for step in sends)
RELAYED = tuple(step for step in ORDER if step[0] != 0 and step[1] != 0)


def split2(value):
    high = value.astype(jnp.bfloat16)
    low = (value - high.astype(jnp.float32)).astype(jnp.bfloat16)
    return high, low


def mm(left, right):
    return jnp.dot(left, right, preferred_element_type=jnp.float32)


def scope(name):
    return jax.named_scope(name)


def kernel(
    feat_hbm, hub_hbm, slot_hbm, nbr_hbm, cnt_hbm, halo_hbm, weight_hbm, bias_hbm,
    out_ref,
    feat, hub, slot, nbr, cnt, halo, weight, bias,
    fhi, base, table, ghi, glo, stage, recv, relay,
    part, part_in, pair_sum, z_in, z_sum, plane_in,
    marks, recip, hub_mark, links_own, links_far, total, w_hi, w_lo,
    in_sem, halo_send, halo_recv, relay_send, relay_recv, a_sem, b_send, b_recv, c_send, c_recv, others_in,
):
    g, l = lax.axis_index("grp"), lax.axis_index("loc")
    y, xh, c = l // 4, (l // 2) % 2, l % 2
    xl, z = g // 4, g % 4
    x = xh * 2 + xl

    def loc_of(dy, dx, dc):
        return ((y + dy + 2 * c * dy) % NY) * 4 + ((xh + dx) % NXH) * 2 + (c + dc) % NC

    def loc_from(dy, dx, dc):
        source = (c + dc) % NC
        return ((y - dy - 2 * source * dy + 3 * NY) % NY) * 4 + ((xh + dx) % NXH) * 2 + source

    def plane_of(dx, dy):
        tx, ty = (x + dx) % 4, (y + dy) % NY
        return (tx % 2) * 4 + z, ty * 4 + (tx // 2) * 2 + c

    quarter = [pl.ds(start, 256) for start in range(0, ROWS, 256)]
    loads = []
    for number, (source, target) in enumerate((
        *((feat_hbm.at[q], feat.at[q]) for q in quarter), (weight_hbm, weight), (halo_hbm, halo),
        (hub_hbm, hub), (nbr_hbm, nbr), (cnt_hbm, cnt), (bias_hbm, bias), (slot_hbm, slot),
    )):
        copy = pltpu.make_async_copy(source, target, in_sem.at[number])
        copy.start()
        loads.append(copy)

    def signal(semaphore, where):
        pl.semaphore_signal(semaphore, inc=1, device_id=where, device_id_type=MESH)

    barrier = pltpu.get_barrier_semaphore()
    beside = (plane_of(1, 0), plane_of(3, 0), plane_of(2, 0))
    greeted = [(g, loc_of(*step)) for step in ORDER if step != (0, 0, 0) and step not in RELAYED]
    greeted += beside[:2]
    for where in greeted:
        signal(barrier, where)
    ring = [(z + dz) % NZ for dz in range(1, NZ)]
    for to in ring:

        @pl.when((z != 0) & (to != 0))
        def _():
            signal(barrier, (xl * 4 + to, l))

    with scope("inputs"):
        loads[4].wait()
        w_hi[...], w_lo[...] = split2(weight[...])
        for copy in loads[:4]:
            copy.wait()

    def weighed(value):
        high, low = split2(value)
        return high, mm(high, w_hi[...]) + mm(low, w_hi[...]) + mm(high, w_lo[...])

    with scope("fw"):
        for start in range(0, ROWS, 256):
            rows = slice(start, start + 256)
            fhi[rows, :], value = weighed(feat[rows, :])
            for half in range(2):
                table[pl.ds(2 * start + half, 256, stride=2), :] = value[:, half * 128 : (half + 1) * 128]
        loads[5].wait()

    halo_copies, relay_copies, sent = {}, {}, []

    by_row = table.reshape(ROWS, 2, 128)

    def gather(number):
        step = ORDER[number]
        peer = loc_of(*step)
        target = recv if step == (0, 0, 0) else stage
        for row in range(SENT):
            target[number, row] = by_row[halo[peer, row]]

    def start_copy(source, target, send_sem, recv_sem, where):
        copy = pltpu.make_async_remote_copy(
            src_ref=source, dst_ref=target, send_sem=send_sem, recv_sem=recv_sem,
            device_id=(g, where), device_id_type=MESH,
        )
        copy.start()
        sent.append(copy)
        return copy

    def send(step):
        number = ORDER.index(step)
        if step in RELAYED:
            at = RELAYED.index(step)
            relay_copies[step] = start_copy(
                stage.at[number], relay.at[at], halo_send.at[number], relay_recv.at[at],
                loc_of(0, 1, 0),
            )
        elif step != (0, 0, 0):
            halo_copies[step] = start_copy(
                stage.at[number], recv.at[number], halo_send.at[number], halo_recv.at[number],
                loc_of(*step),
            )

    def forward(step):
        number, at = ORDER.index(step), RELAYED.index(step)
        with scope(f"relay{step[0]}{step[2]}"):
            relay_copies[step].wait_recv()
        halo_copies[step] = start_copy(
            relay.at[at], recv.at[number], relay_send.at[at], halo_recv.at[number],
            loc_of(step[0], 0, step[2]),
        )

    def exchange(stage_number):
        for step in PLAN[stage_number][0]:
            if stage_number < 3 and step != ORDER[0]:
                gather(ORDER.index(step))
            send(step)
        for step in PLAN[stage_number][1]:
            forward(step)

    with scope("gather0"):
        gather(0)
    with scope("barrier"):
        pl.semaphore_wait(barrier, len(greeted) + jnp.where(z == 0, 0, NZ - 1))
    exchange(0)

    for to in ring:

        @pl.when((z == 0) | (to == 0))
        def _():
            signal(barrier, (xl * 4 + to, l))

    for number, where in enumerate(beside):
        signal(others_in.at[number], where)

    with scope("gather1"):
        exchange(1)

    with scope("hubpart"):
        loads[6].wait()
        upper = lax.broadcasted_iota(jnp.int32, (128, 128), 0) % 8 < 4
        for start in range(0, HUBS, 128):
            rows = mm(hub[start : start + 128, :], fhi[...])
            left, right = rows[:, :128], rows[:, 128:]
            part[0, start : start + 128, :] = jnp.where(upper, left, pltpu.roll(right, 4, 0))
            part[1, start : start + 128, :] = jnp.where(upper, pltpu.roll(left, 124, 0), right)
        pair_copy = pltpu.make_async_remote_copy(
            src_ref=part.at[1 - c],
            dst_ref=part_in,
            send_sem=a_sem.at[0],
            recv_sem=a_sem.at[1],
            device_id=(g, loc_of(0, 0, 1)),
            device_id_type=MESH,
        )
        pair_copy.start()

    with scope("gather2"):
        exchange(2)
        for number in range(sum(len(sends) for sends, _ in PLAN[:3]), len(ORDER)):
            gather(number)

    with scope("a_to_b"):
        pair_copy.wait_recv()
        pair_sum[...] = (part[pl.ds(c, 1)][0] + part_in[...]).reshape(NXL, NZ, 64, 128)
        z_copies = []

        @pl.when(z == 0)
        def _():
            pl.semaphore_wait(barrier, NZ - 1)

        for dz in range(1, NZ):
            to = (z + dz) % NZ
            copy = pltpu.make_async_remote_copy(
                src_ref=pair_sum.at[:, to],
                dst_ref=z_in.at[dz - 1],
                send_sem=b_send.at[dz - 1],
                recv_sem=b_recv.at[dz - 1],
                device_id=(xl * 4 + to, l),
                device_id_type=MESH,
            )
            copy.start()
            z_copies.append(copy)


    with scope("marks"):
        loads[7].wait()
        loads[8].wait()
        slots, used = nbr[...], cnt[...]
        active = lax.broadcasted_iota(jnp.int32, (SLOTS, ROWS), 0) < used
        place = slots & (FIELD_ROWS - 1)
        one = jnp.where(active, jnp.left_shift(1, (slots >> 9) * FIELD_BITS), 0)
        inverse = jnp.broadcast_to(1.0 / used.astype(jnp.float32), (8, ROWS))
        for start in range(0, ROWS, 128):
            rows = slice(start, start + 128)
            marks[0, rows, :] = place[:, rows].T
            marks[1, rows, :] = one[:, rows].T
            recip[rows, :] = inverse[:, rows].T

    pool_lane = lax.broadcasted_iota(jnp.int32, (32, FIELD_ROWS), 1)

    def build(block, carry):
        rows = pl.ds(pl.multiple_of(block * 32, 32), 32)
        row_place, row_one = marks[0, rows, :], marks[1, rows, :]
        packed = jnp.zeros((32, FIELD_ROWS), jnp.int32)
        for k in range(SLOTS):
            packed = packed + jnp.where(
                row_place[:, k : k + 1] == pool_lane, row_one[:, k : k + 1], 0
            )
        for field in range(FIELDS):
            number = (packed >> (field * FIELD_BITS)) & (2**FIELD_BITS - 1)
            number = number.astype(jnp.float32).astype(jnp.bfloat16)
            if field < 2:
                links_own[2 * field, rows, :] = number[:, :256]
                links_own[2 * field + 1, rows, :] = number[:, 256:]
            else:
                for peer in range(4):
                    links = number[:, peer * SENT : (peer + 1) * SENT]
                    for half in range(2):
                        lanes = slice(half * SENT, (half + 1) * SENT)
                        links_far[(field - 2) * 4 + peer, rows, lanes] = links
        return carry

    exchange(3)
    with scope("build1"):
        lax.fori_loop(0, 8, build, 0)
    exchange(4)
    with scope("build2"):
        lax.fori_loop(8, 16, build, 0)
    exchange(5)
    with scope("build3"):
        lax.fori_loop(16, 24, build, 0)
    exchange(6)
    with scope("b_to_c"):
        for copy in z_copies:
            copy.wait_recv()
        for half in range(NXL):
            value = pair_sum[half, pl.ds(z, 1)][0]
            for dz in range(NZ - 1):
                value = value + z_in[dz, half]
            z_sum[half] = value.reshape(8, 8, 128)
        plane_copies = []
        for number in range(3):
            pl.semaphore_wait(others_in.at[number], 1)
        for dx in range(4):
            for dy in range(NY):
                if (dx, dy) == (0, 0):
                    continue
                tx, ty = (x + dx) % 4, (y + dy) % NY
                copy = pltpu.make_async_remote_copy(
                    src_ref=z_sum.at[tx % 2, ty * 2 + tx // 2],
                    dst_ref=plane_in.at[dx * 4 + dy],
                    send_sem=c_send.at[dx * 4 + dy],
                    recv_sem=c_recv.at[dx * 4 + dy],
                    device_id=plane_of(dx, dy),
                    device_id_type=MESH,
                )
                copy.start()
                plane_copies.append(copy)

    exchange(7)
    with scope("build4"):
        lax.fori_loop(24, 32, build, 0)
    exchange(8)

    with scope("hub_mark"):
        loads[9].wait()
        loads[10].wait()
        vertex = lax.broadcasted_iota(jnp.int32, (ROWS, 128), 0)
        lane = lax.broadcasted_iota(jnp.int32, (ROWS, 128), 1)
        mark = jnp.zeros((ROWS, 128), jnp.float32)
        for r in range(HUB_OWN):
            mark = jnp.where((vertex == slot[r]) & ((lane == r) | (lane == 4 + r)), 1.0, mark)
        hub_mark[...] = mark.astype(jnp.bfloat16)
        for start in range(0, ROWS, 256):
            rows = slice(start, start + 256)
            halves = [table[pl.ds(2 * start + half, 256, stride=2), :] for half in range(2)]
            value = jnp.concatenate(halves, axis=1)
            base[rows, :] = value + bias[...]
            ghi[rows, :], glo[rows, :] = split2(value)

    with scope("own"):
        for number in range(4):
            rows = slice(number * 256, (number + 1) * 256)
            value = mm(links_own[number], ghi[rows, :]) + mm(links_own[number], glo[rows, :])
            total[...] = value if number == 0 else total[...] + value

    def far(step):
        number = ORDER.index(step)
        dy, dx, dc = step
        if step != (0, 0, 0):
            with scope(f"wait{dy}{dx}{dc}"):
                halo_copies[step].wait_recv()
        peer = loc_from(dy, dx, dc)
        halves = [recv[number, :, half, :] for half in range(2)]
        high, low = split2(jnp.concatenate(halves, axis=1))
        return peer, jnp.concatenate([high, low], axis=0)

    def linked(peer, rows):
        return links_far[pl.ds(peer, 1), rows, :][0]

    def hub_rows():
        with scope("wait_c"):
            for copy in plane_copies:
                copy.wait_recv()
        with scope("hub_rows"):
            hub_tile = z_sum[pl.ds(xl, 1), pl.ds(y * 2 + xh, 1)][0, 0]
            for source in range(1, 16):
                hub_tile = hub_tile + plane_in[source]
            hub_own = weighed(jnp.concatenate([hub_tile, pltpu.roll(hub_tile, 4, 0)], axis=1))[1]
            upper = lax.broadcasted_iota(jnp.int32, (8, WIDTH), 0) < HUB_OWN
            high = hub_own.astype(jnp.bfloat16).astype(jnp.float32)
            both = jnp.where(upper, high, pltpu.roll(hub_own - high, 4, 0))
            hub_values = jnp.concatenate([both, jnp.zeros((120, WIDTH), jnp.float32)], axis=0)
            hub_values = hub_values.astype(jnp.bfloat16)
            base[...] += mm(hub_mark[...], hub_values)

    for kind, step in TAKE_ORDER:
        if kind == "hub":
            hub_rows()
        elif kind == "forward":
            forward(step)
        elif kind == "take":
            peer, values = far(step)
            with scope("take"):
                total[...] += mm(linked(peer, slice(None)), values)

    with scope("combine"):
        base[...] += total[...] * recip[:, 0:1]
    last = [far(step) for kind, step in TAKE_ORDER if kind == "last"]
    with scope("final"):
        for start in range(0, ROWS, 256):
            rows = slice(start, start + 256)
            value = sum(mm(linked(peer, rows), values) for peer, values in last)
            out_ref[rows, :] = jnp.maximum(base[rows, :] + value * recip[rows, 0:1], 0.0)

    with scope("wait_send"):
        for copy in sent:
            copy.wait_send()
        pair_copy.wait_send()
        for copy in z_copies + plane_copies:
            copy.wait_send()


def on_device(features, hub_block, hub_slot, neighbours, counts, halo_send, weight, bias):
    f32, bf16, i32 = jnp.float32, jnp.bfloat16, jnp.int32
    vmem, dma = pltpu.VMEM, pltpu.SemaphoreType.DMA
    return pl.pallas_call(
        kernel,
        out_shape=jax.ShapeDtypeStruct((ROWS, WIDTH), f32),
        in_specs=[pl.BlockSpec(memory_space=pltpu.HBM)] * 8,
        out_specs=pl.BlockSpec(memory_space=pltpu.VMEM),
        scratch_shapes=[
            vmem((ROWS, WIDTH), f32),
            vmem((HUBS, ROWS), bf16),
            pltpu.SMEM((HUB_OWN,), i32),
            vmem((SLOTS, ROWS), i32),
            vmem((1, ROWS), i32),
            pltpu.SMEM((16, SENT), i32),
            vmem((WIDTH, WIDTH), f32),
            vmem((1, WIDTH), f32),
            vmem((ROWS, WIDTH), bf16),
            vmem((ROWS, WIDTH), f32),
            vmem((2 * ROWS, 128), f32),
            vmem((ROWS, WIDTH), bf16),
            vmem((ROWS, WIDTH), bf16),
            vmem((16, SENT, 2, 128), f32),
            vmem((16, SENT, 2, 128), f32),
            vmem((6, SENT, 2, 128), f32),
            vmem((NC, HUBS, 128), f32),
            vmem((HUBS, 128), f32),
            vmem((NXL, NZ, 64, 128), f32),
            vmem((NZ - 1, NXL, 64, 128), f32),
            vmem((NXL, 8, 8, 128), f32),
            vmem((16, 8, 128), f32),
            vmem((2, ROWS, SLOTS), i32),
            vmem((ROWS, 8), f32),
            vmem((ROWS, 128), bf16),
            vmem((4, ROWS, 256), bf16),
            vmem((16, ROWS, 2 * SENT), bf16),
            vmem((ROWS, WIDTH), f32),
            vmem((WIDTH, WIDTH), bf16),
            vmem((WIDTH, WIDTH), bf16),
            dma((11,)), dma((16,)), dma((16,)), dma((6,)), dma((6,)), dma((2,)),
            dma((3,)), dma((3,)), dma((16,)), dma((16,)), pltpu.SemaphoreType.REGULAR((3,)),
        ],
        compiler_params=pltpu.CompilerParams(
            collective_id=0, has_side_effects=True, vmem_limit_bytes=40 * 1024 * 1024
        ),
    )(
        *(
            pltpu.with_memory_space_constraint(array, pltpu.HBM)
            for array in (
                features, hub_block, hub_slot, neighbours.T, counts.reshape(1, -1), halo_send,
                weight, bias.reshape(1, -1),
            )
        )
    )


def solution(mesh):
    in_specs = (
        P(("grp", "loc"), None),
        P(None, ("grp", "loc")),
        P(("grp", "loc")),
        P(("grp", "loc"), None),
        P(("grp", "loc")),
        P(("grp", "loc"), None),
        P(),
        P(),
    )
    out_specs = P(("grp", "loc"), None)
    return jax.shard_map(
        on_device, mesh=mesh, in_specs=in_specs, out_specs=out_specs, check_vma=False
    )
```

```python
import jax
import jax.numpy as jnp
from jax import lax
from jax.experimental import pallas as pl
from jax.experimental.pallas import tpu as pltpu
from jax.sharding import PartitionSpec as P

MESH = pl.DeviceIdType.MESH
NY, NXH, NC, NXL, NZ = 4, 2, 2, 2, 4
ROWS, WIDTH, SLOTS, SENT = 1024, 256, 16, 128
HUBS, HUB_OWN = 512, 4
FIELD_ROWS, FIELDS, FIELD_BITS = 512, 6, 5

PLAN = (
    (((2, 1, 0), ), ()),
    (((1, 0, 0), (2, 1, 1), (3, 0, 0), ), ()),
    (((1, 1, 0), (2, 0, 0), (3, 1, 0), (2, 0, 1), (1, 0, 1), (3, 0, 1), (0, 0, 1), (0, 0, 0), ), ()),
    (((1, 1, 1), (3, 1, 1), ), ()),
    ((), ((2, 1, 0), )),
    ((), ((2, 1, 1), )),
    ((), ()),
    (((0, 1, 0), (0, 1, 1), ), ()),
    ((), ((1, 1, 0), )),
)
TAKE_ORDER = (
    ("take", (0, 0, 0)), ("take", (0, 0, 1)), ("forward", (3, 1, 0)),
    ("take", (1, 0, 0)), ("take", (3, 0, 0)), ("take", (2, 0, 0)),
    ("forward", (1, 1, 1)), ("take", (2, 0, 1)), ("take", (1, 0, 1)),
    ("take", (3, 0, 1)), ("take", (2, 1, 0)), ("forward", (3, 1, 1)),
    ("take", (2, 1, 1)), ("take", (1, 1, 0)), ("hub", (0, 0, 0)),
    ("take", (0, 1, 0)), ("take", (3, 1, 0)), ("take", (0, 1, 1)),
    ("last", (1, 1, 1)), ("last", (3, 1, 1)),
)


ORDER = tuple(step for sends, _ in PLAN for step in sends)
RELAYED = tuple(step for step in ORDER if step[0] != 0 and step[1] != 0)


def split2(value):
    high = value.astype(jnp.bfloat16)
    low = (value - high.astype(jnp.float32)).astype(jnp.bfloat16)
    return high, low


def mm(left, right):
    return jnp.dot(left, right, preferred_element_type=jnp.float32)


def scope(name):
    return jax.named_scope(name)


def kernel(
    feat_hbm, hub_hbm, slot_hbm, nbr_hbm, cnt_hbm, halo_hbm, weight_hbm, bias_hbm,
    out_ref,
    feat, hub, slot, nbr, cnt, halo, weight, bias,
    fhi, base, table, ghi, glo, stage, recv, relay,
    part, part_in, pair_sum, z_in, z_sum, plane_in,
    marks, recip, hub_mark, links_own, links_far, total, w_hi, w_lo,
    in_sem, halo_send, halo_recv, relay_send, relay_recv, a_sem, b_send, b_recv, c_send, c_recv, others_in,
):
    g, l = lax.axis_index("grp"), lax.axis_index("loc")
    y, xh, c = l // 4, (l // 2) % 2, l % 2
    xl, z = g // 4, g % 4
    x = xh * 2 + xl

    def loc_of(dy, dx, dc):
        return ((y + dy + 2 * c * dy) % NY) * 4 + ((xh + dx) % NXH) * 2 + (c + dc) % NC

    def loc_from(dy, dx, dc):
        source = (c + dc) % NC
        return ((y - dy - 2 * source * dy + 3 * NY) % NY) * 4 + ((xh + dx) % NXH) * 2 + source

    def plane_of(dx, dy):
        tx, ty = (x + dx) % 4, (y + dy) % NY
        return (tx % 2) * 4 + z, ty * 4 + (tx // 2) * 2 + c

    quarter = [pl.ds(start, 256) for start in range(0, ROWS, 256)]
    loads = []
    for number, (source, target) in enumerate((
        *((feat_hbm.at[q], feat.at[q]) for q in quarter), (weight_hbm, weight), (halo_hbm, halo),
        (hub_hbm, hub), (nbr_hbm, nbr), (cnt_hbm, cnt), (bias_hbm, bias), (slot_hbm, slot),
    )):
        copy = pltpu.make_async_copy(source, target, in_sem.at[number])
        copy.start()
        loads.append(copy)

    def signal(semaphore, where):
        pl.semaphore_signal(semaphore, inc=1, device_id=where, device_id_type=MESH)

    barrier = pltpu.get_barrier_semaphore()
    beside = (plane_of(1, 0), plane_of(3, 0), plane_of(2, 0))
    greeted = [(g, loc_of(*step)) for step in ORDER if step != (0, 0, 0) and step not in RELAYED]
    greeted += beside[:2]
    for where in greeted:
        signal(barrier, where)
    ring = [(z + dz) % NZ for dz in range(1, NZ)]
    for to in ring:

        @pl.when((z != 0) & (to != 0))
        def _():
            signal(barrier, (xl * 4 + to, l))

    with scope("inputs"):
        loads[4].wait()
        w_hi[...], w_lo[...] = split2(weight[...])
        for copy in loads[:4]:
            copy.wait()

    def weighed(value):
        high, low = split2(value)
        return high, mm(high, w_hi[...]) + mm(low, w_hi[...]) + mm(high, w_lo[...])

    with scope("fw"):
        for start in range(0, ROWS, 256):
            rows = slice(start, start + 256)
            fhi[rows, :], value = weighed(feat[rows, :])
            for half in range(2):
                table[pl.ds(2 * start + half, 256, stride=2), :] = value[:, half * 128 : (half + 1) * 128]
        loads[5].wait()

    halo_copies, relay_copies, sent = {}, {}, []

    by_row = table.reshape(ROWS, 2, 128)

    def gather(number):
        step = ORDER[number]
        peer = loc_of(*step)
        target = recv if step == (0, 0, 0) else stage
        for row in range(SENT):
            target[number, row] = by_row[halo[peer, row]]

    def start_copy(source, target, send_sem, recv_sem, where):
        copy = pltpu.make_async_remote_copy(
            src_ref=source, dst_ref=target, send_sem=send_sem, recv_sem=recv_sem,
            device_id=(g, where), device_id_type=MESH,
        )
        copy.start()
        sent.append(copy)
        return copy

    def send(step):
        number = ORDER.index(step)
        if step in RELAYED:
            at = RELAYED.index(step)
            relay_copies[step] = start_copy(
                stage.at[number], relay.at[at], halo_send.at[number], relay_recv.at[at],
                loc_of(0, 1, 0),
            )
        elif step != (0, 0, 0):
            halo_copies[step] = start_copy(
                stage.at[number], recv.at[number], halo_send.at[number], halo_recv.at[number],
                loc_of(*step),
            )

    def forward(step):
        number, at = ORDER.index(step), RELAYED.index(step)
        with scope(f"relay{step[0]}{step[2]}"):
            relay_copies[step].wait_recv()
        halo_copies[step] = start_copy(
            relay.at[at], recv.at[number], relay_send.at[at], halo_recv.at[number],
            loc_of(step[0], 0, step[2]),
        )

    def exchange(stage_number):
        for step in PLAN[stage_number][0]:
            if stage_number < 3 and step != ORDER[0]:
                gather(ORDER.index(step))
            send(step)
        for step in PLAN[stage_number][1]:
            forward(step)

    with scope("gather0"):
        gather(0)
    with scope("barrier"):
        pl.semaphore_wait(barrier, len(greeted) + jnp.where(z == 0, 0, NZ - 1))
    exchange(0)

    for to in ring:

        @pl.when((z == 0) | (to == 0))
        def _():
            signal(barrier, (xl * 4 + to, l))

    for number, where in enumerate(beside):
        signal(others_in.at[number], where)

    with scope("gather1"):
        exchange(1)

    with scope("hubpart"):
        loads[6].wait()
        upper = lax.broadcasted_iota(jnp.int32, (128, 128), 0) % 8 < 4
        for start in range(0, HUBS, 128):
            rows = mm(hub[start : start + 128, :], fhi[...])
            left, right = rows[:, :128], rows[:, 128:]
            part[0, start : start + 128, :] = jnp.where(upper, left, pltpu.roll(right, 4, 0))
            part[1, start : start + 128, :] = jnp.where(upper, pltpu.roll(left, 124, 0), right)
        pair_copy = pltpu.make_async_remote_copy(
            src_ref=part.at[1 - c],
            dst_ref=part_in,
            send_sem=a_sem.at[0],
            recv_sem=a_sem.at[1],
            device_id=(g, loc_of(0, 0, 1)),
            device_id_type=MESH,
        )
        pair_copy.start()

    with scope("gather2"):
        exchange(2)
        for number in range(sum(len(sends) for sends, _ in PLAN[:3]), len(ORDER)):
            gather(number)

    with scope("a_to_b"):
        pair_copy.wait_recv()
        pair_sum[...] = (part[pl.ds(c, 1)][0] + part_in[...]).reshape(NXL, NZ, 64, 128)
        z_copies = []

        @pl.when(z == 0)
        def _():
            pl.semaphore_wait(barrier, NZ - 1)

        for dz in range(1, NZ):
            to = (z + dz) % NZ
            copy = pltpu.make_async_remote_copy(
                src_ref=pair_sum.at[:, to],
                dst_ref=z_in.at[dz - 1],
                send_sem=b_send.at[dz - 1],
                recv_sem=b_recv.at[dz - 1],
                device_id=(xl * 4 + to, l),
                device_id_type=MESH,
            )
            copy.start()
            z_copies.append(copy)


    with scope("marks"):
        loads[7].wait()
        loads[8].wait()
        slots, used = nbr[...], cnt[...]
        active = lax.broadcasted_iota(jnp.int32, (SLOTS, ROWS), 0) < used
        place = slots & (FIELD_ROWS - 1)
        one = jnp.where(active, jnp.left_shift(1, (slots >> 9) * FIELD_BITS), 0)
        inverse = jnp.broadcast_to(1.0 / used.astype(jnp.float32), (8, ROWS))
        for start in range(0, ROWS, 128):
            rows = slice(start, start + 128)
            marks[0, rows, :] = place[:, rows].T
            marks[1, rows, :] = one[:, rows].T
            recip[rows, :] = inverse[:, rows].T

    pool_lane = lax.broadcasted_iota(jnp.int32, (32, FIELD_ROWS), 1)

    def build(block, carry):
        rows = pl.ds(pl.multiple_of(block * 32, 32), 32)
        row_place, row_one = marks[0, rows, :], marks[1, rows, :]
        packed = jnp.zeros((32, FIELD_ROWS), jnp.int32)
        for k in range(SLOTS):
            packed = packed + jnp.where(
                row_place[:, k : k + 1] == pool_lane, row_one[:, k : k + 1], 0
            )
        for field in range(FIELDS):
            number = (packed >> (field * FIELD_BITS)) & (2**FIELD_BITS - 1)
            number = number.astype(jnp.float32).astype(jnp.bfloat16)
            if field < 2:
                links_own[2 * field, rows, :] = number[:, :256]
                links_own[2 * field + 1, rows, :] = number[:, 256:]
            else:
                for peer in range(4):
                    links = number[:, peer * SENT : (peer + 1) * SENT]
                    for half in range(2):
                        lanes = slice(half * SENT, (half + 1) * SENT)
                        links_far[(field - 2) * 4 + peer, rows, lanes] = links
        return carry

    exchange(3)
    with scope("build1"):
        lax.fori_loop(0, 8, build, 0)
    exchange(4)
    with scope("build2"):
        lax.fori_loop(8, 16, build, 0)
    exchange(5)
    with scope("build3"):
        lax.fori_loop(16, 24, build, 0)
    exchange(6)
    with scope("b_to_c"):
        for copy in z_copies:
            copy.wait_recv()
        for half in range(NXL):
            value = pair_sum[half, pl.ds(z, 1)][0]
            for dz in range(NZ - 1):
                value = value + z_in[dz, half]
            z_sum[half] = value.reshape(8, 8, 128)
        plane_copies = []
        for number in range(3):
            pl.semaphore_wait(others_in.at[number], 1)
        for dx in range(4):
            for dy in range(NY):
                if (dx, dy) == (0, 0):
                    continue
                tx, ty = (x + dx) % 4, (y + dy) % NY
                copy = pltpu.make_async_remote_copy(
                    src_ref=z_sum.at[tx % 2, ty * 2 + tx // 2],
                    dst_ref=plane_in.at[dx * 4 + dy],
                    send_sem=c_send.at[dx * 4 + dy],
                    recv_sem=c_recv.at[dx * 4 + dy],
                    device_id=plane_of(dx, dy),
                    device_id_type=MESH,
                )
                copy.start()
                plane_copies.append(copy)

    exchange(7)
    with scope("build4"):
        lax.fori_loop(24, 32, build, 0)
    exchange(8)

    with scope("hub_mark"):
        loads[9].wait()
        loads[10].wait()
        vertex = lax.broadcasted_iota(jnp.int32, (ROWS, 128), 0)
        lane = lax.broadcasted_iota(jnp.int32, (ROWS, 128), 1)
        mark = jnp.zeros((ROWS, 128), jnp.float32)
        for r in range(HUB_OWN):
            mark = jnp.where((vertex == slot[r]) & ((lane == r) | (lane == 4 + r)), 1.0, mark)
        hub_mark[...] = mark.astype(jnp.bfloat16)
        for start in range(0, ROWS, 256):
            rows = slice(start, start + 256)
            halves = [table[pl.ds(2 * start + half, 256, stride=2), :] for half in range(2)]
            value = jnp.concatenate(halves, axis=1)
            base[rows, :] = value + bias[...]
            ghi[rows, :], glo[rows, :] = split2(value)

    with scope("own"):
        for number in range(4):
            rows = slice(number * 256, (number + 1) * 256)
            value = mm(links_own[number], ghi[rows, :]) + mm(links_own[number], glo[rows, :])
            total[...] = value if number == 0 else total[...] + value

    def far(step):
        number = ORDER.index(step)
        dy, dx, dc = step
        if step != (0, 0, 0):
            with scope(f"wait{dy}{dx}{dc}"):
                halo_copies[step].wait_recv()
        peer = loc_from(dy, dx, dc)
        halves = [recv[number, :, half, :] for half in range(2)]
        high, low = split2(jnp.concatenate(halves, axis=1))
        return peer, jnp.concatenate([high, low], axis=0)

    def linked(peer, rows):
        return links_far[pl.ds(peer, 1), rows, :][0]

    def hub_rows():
        with scope("wait_c"):
            for copy in plane_copies:
                copy.wait_recv()
        with scope("hub_rows"):
            hub_tile = z_sum[pl.ds(xl, 1), pl.ds(y * 2 + xh, 1)][0, 0]
            for source in range(1, 16):
                hub_tile = hub_tile + plane_in[source]
            hub_own = weighed(jnp.concatenate([hub_tile, pltpu.roll(hub_tile, 4, 0)], axis=1))[1]
            upper = lax.broadcasted_iota(jnp.int32, (8, WIDTH), 0) < HUB_OWN
            high = hub_own.astype(jnp.bfloat16).astype(jnp.float32)
            both = jnp.where(upper, high, pltpu.roll(hub_own - high, 4, 0))
            hub_values = jnp.concatenate([both, jnp.zeros((120, WIDTH), jnp.float32)], axis=0)
            hub_values = hub_values.astype(jnp.bfloat16)
            base[...] += mm(hub_mark[...], hub_values)

    for kind, step in TAKE_ORDER:
        if kind == "hub":
            hub_rows()
        elif kind == "forward":
            forward(step)
        elif kind == "take":
            peer, values = far(step)
            with scope("take"):
                total[...] += mm(linked(peer, slice(None)), values)

    with scope("combine"):
        base[...] += total[...] * recip[:, 0:1]
    last = [far(step) for kind, step in TAKE_ORDER if kind == "last"]
    with scope("final"):
        for start in range(0, ROWS, 256):
            rows = slice(start, start + 256)
            value = sum(mm(linked(peer, rows), values) for peer, values in last)
            out_ref[rows, :] = jnp.maximum(base[rows, :] + value * recip[rows, 0:1], 0.0)

    with scope("wait_send"):
        for copy in sent:
            copy.wait_send()
        pair_copy.wait_send()
        for copy in z_copies + plane_copies:
            copy.wait_send()


def on_device(features, hub_block, hub_slot, neighbours, counts, halo_send, weight, bias):
    f32, bf16, i32 = jnp.float32, jnp.bfloat16, jnp.int32
    vmem, dma = pltpu.VMEM, pltpu.SemaphoreType.DMA
    return pl.pallas_call(
        kernel,
        out_shape=jax.ShapeDtypeStruct((ROWS, WIDTH), f32),
        in_specs=[pl.BlockSpec(memory_space=pltpu.HBM)] * 8,
        out_specs=pl.BlockSpec(memory_space=pltpu.VMEM),
        scratch_shapes=[
            vmem((ROWS, WIDTH), f32),
            vmem((HUBS, ROWS), bf16),
            pltpu.SMEM((HUB_OWN,), i32),
            vmem((SLOTS, ROWS), i32),
            vmem((1, ROWS), i32),
            pltpu.SMEM((16, SENT), i32),
            vmem((WIDTH, WIDTH), f32),
            vmem((1, WIDTH), f32),
            vmem((ROWS, WIDTH), bf16),
            vmem((ROWS, WIDTH), f32),
            vmem((2 * ROWS, 128), f32),
            vmem((ROWS, WIDTH), bf16),
            vmem((ROWS, WIDTH), bf16),
            vmem((16, SENT, 2, 128), f32),
            vmem((16, SENT, 2, 128), f32),
            vmem((6, SENT, 2, 128), f32),
            vmem((NC, HUBS, 128), f32),
            vmem((HUBS, 128), f32),
            vmem((NXL, NZ, 64, 128), f32),
            vmem((NZ - 1, NXL, 64, 128), f32),
            vmem((NXL, 8, 8, 128), f32),
            vmem((16, 8, 128), f32),
            vmem((2, ROWS, SLOTS), i32),
            vmem((ROWS, 8), f32),
            vmem((ROWS, 128), bf16),
            vmem((4, ROWS, 256), bf16),
            vmem((16, ROWS, 2 * SENT), bf16),
            vmem((ROWS, WIDTH), f32),
            vmem((WIDTH, WIDTH), bf16),
            vmem((WIDTH, WIDTH), bf16),
            dma((11,)), dma((16,)), dma((16,)), dma((6,)), dma((6,)), dma((2,)),
            dma((3,)), dma((3,)), dma((16,)), dma((16,)), pltpu.SemaphoreType.REGULAR((3,)),
        ],
        compiler_params=pltpu.CompilerParams(
            collective_id=0, has_side_effects=True, vmem_limit_bytes=40 * 1024 * 1024
        ),
    )(
        *(
            pltpu.with_memory_space_constraint(array, pltpu.HBM)
            for array in (
                features, hub_block, hub_slot, neighbours.T, counts.reshape(1, -1), halo_send,
                weight, bias.reshape(1, -1),
            )
        )
    )


def solution(mesh):
    in_specs = (
        P(("grp", "loc"), None),
        P(None, ("grp", "loc")),
        P(("grp", "loc")),
        P(("grp", "loc"), None),
        P(("grp", "loc")),
        P(("grp", "loc"), None),
        P(),
        P(),
    )
    out_specs = P(("grp", "loc"), None)
    return jax.shard_map(
        on_device, mesh=mesh, in_specs=in_specs, out_specs=out_specs, check_vma=False
    )
```

```python
import jax
import jax.numpy as jnp
from jax import lax
from jax.experimental import pallas as pl
from jax.experimental.pallas import tpu as pltpu
from jax.sharding import PartitionSpec as P

MESH = pl.DeviceIdType.MESH
NY, NXH, NC, NXL, NZ = 4, 2, 2, 2, 4
ROWS, WIDTH, SLOTS, SENT = 1024, 256, 16, 128
HUBS, HUB_OWN = 512, 4
FIELD_ROWS, FIELDS, FIELD_BITS = 512, 6, 5

PLAN = (
    (((2, 1, 0), ), ()),
    (((1, 0, 0), (2, 1, 1), (3, 0, 0), ), ()),
    (((1, 1, 0), (2, 0, 0), (3, 1, 0), (2, 0, 1), (1, 0, 1), (3, 0, 1), (0, 0, 1), (0, 0, 0), ), ()),
    (((1, 1, 1), (3, 1, 1), ), ()),
    ((), ((2, 1, 0), )),
    ((), ((2, 1, 1), )),
    ((), ()),
    (((0, 1, 0), (0, 1, 1), ), ()),
    ((), ((1, 1, 0), )),
)
TAKE_ORDER = (
    ("take", (0, 0, 0)), ("take", (0, 0, 1)), ("forward", (3, 1, 0)),
    ("take", (1, 0, 0)), ("take", (3, 0, 0)), ("take", (2, 0, 0)),
    ("forward", (1, 1, 1)), ("take", (2, 0, 1)), ("take", (1, 0, 1)),
    ("take", (3, 0, 1)), ("take", (2, 1, 0)), ("forward", (3, 1, 1)),
    ("take", (2, 1, 1)), ("take", (1, 1, 0)), ("hub", (0, 0, 0)),
    ("take", (0, 1, 0)), ("take", (3, 1, 0)), ("take", (0, 1, 1)),
    ("last", (1, 1, 1)), ("last", (3, 1, 1)),
)


ORDER = tuple(step for sends, _ in PLAN for step in sends)
LAST = sum(kind == "last" for kind, _ in TAKE_ORDER)
RELAYED = tuple(step for step in ORDER if step[0] != 0 and step[1] != 0)


def split2(value):
    high = value.astype(jnp.bfloat16)
    low = (value - high.astype(jnp.float32)).astype(jnp.bfloat16)
    return high, low


def mm(left, right):
    return jnp.dot(left, right, preferred_element_type=jnp.float32)


def scope(name):
    return jax.named_scope(name)


def kernel(
    feat_hbm, hub_hbm, slot_hbm, nbr_hbm, cnt_hbm, halo_hbm, weight_hbm, bias_hbm,
    base, recip, last_links, last_values,
    feat, hub, slot, nbr, cnt, halo, weight, bias,
    fhi, table, ghi, glo, stage, recv, relay,
    part, part_in, pair_sum, z_in, z_sum, plane_in,
    marks, hub_mark, links_own, links_far, total, w_hi, w_lo,
    in_sem, halo_send, halo_recv, relay_send, relay_recv, a_sem, b_send, b_recv, c_send, c_recv, others_in,
):
    g, l = lax.axis_index("grp"), lax.axis_index("loc")
    y, xh, c = l // 4, (l // 2) % 2, l % 2
    xl, z = g // 4, g % 4
    x = xh * 2 + xl

    def loc_of(dy, dx, dc):
        return ((y + dy + 2 * c * dy) % NY) * 4 + ((xh + dx) % NXH) * 2 + (c + dc) % NC

    def loc_from(dy, dx, dc):
        source = (c + dc) % NC
        return ((y - dy - 2 * source * dy + 3 * NY) % NY) * 4 + ((xh + dx) % NXH) * 2 + source

    def plane_of(dx, dy):
        tx, ty = (x + dx) % 4, (y + dy) % NY
        return (tx % 2) * 4 + z, ty * 4 + (tx // 2) * 2 + c

    quarter = [pl.ds(start, 256) for start in range(0, ROWS, 256)]
    loads = []
    for number, (source, target) in enumerate((
        *((feat_hbm.at[q], feat.at[q]) for q in quarter), (weight_hbm, weight), (halo_hbm, halo),
        (hub_hbm, hub), (nbr_hbm, nbr), (cnt_hbm, cnt), (bias_hbm, bias), (slot_hbm, slot),
    )):
        copy = pltpu.make_async_copy(source, target, in_sem.at[number])
        copy.start()
        loads.append(copy)

    def signal(semaphore, where):
        pl.semaphore_signal(semaphore, inc=1, device_id=where, device_id_type=MESH)

    barrier = pltpu.get_barrier_semaphore()
    beside = (plane_of(1, 0), plane_of(3, 0), plane_of(2, 0))
    greeted = [(g, loc_of(*step)) for step in ORDER if step != (0, 0, 0) and step not in RELAYED]
    greeted += beside[:2]
    for where in greeted:
        signal(barrier, where)
    ring = [(z + dz) % NZ for dz in range(1, NZ)]
    for to in ring:

        @pl.when((z != 0) & (to != 0))
        def _():
            signal(barrier, (xl * 4 + to, l))

    with scope("inputs"):
        loads[4].wait()
        w_hi[...], w_lo[...] = split2(weight[...])
        for copy in loads[:4]:
            copy.wait()

    def weighed(value):
        high, low = split2(value)
        return high, mm(high, w_hi[...]) + mm(low, w_hi[...]) + mm(high, w_lo[...])

    with scope("fw"):
        for start in range(0, ROWS, 256):
            rows = slice(start, start + 256)
            fhi[rows, :], value = weighed(feat[rows, :])
            for half in range(2):
                table[pl.ds(2 * start + half, 256, stride=2), :] = value[:, half * 128 : (half + 1) * 128]
        loads[5].wait()

    halo_copies, relay_copies, sent = {}, {}, []

    by_row = table.reshape(ROWS, 2, 128)

    def gather(number):
        step = ORDER[number]
        peer = loc_of(*step)
        target = recv if step == (0, 0, 0) else stage
        for row in range(SENT):
            target[number, row] = by_row[halo[peer, row]]

    def start_copy(source, target, send_sem, recv_sem, where):
        copy = pltpu.make_async_remote_copy(
            src_ref=source, dst_ref=target, send_sem=send_sem, recv_sem=recv_sem,
            device_id=(g, where), device_id_type=MESH,
        )
        copy.start()
        sent.append(copy)
        return copy

    def send(step):
        number = ORDER.index(step)
        if step in RELAYED:
            at = RELAYED.index(step)
            relay_copies[step] = start_copy(
                stage.at[number], relay.at[at], halo_send.at[number], relay_recv.at[at],
                loc_of(0, 1, 0),
            )
        elif step != (0, 0, 0):
            halo_copies[step] = start_copy(
                stage.at[number], recv.at[number], halo_send.at[number], halo_recv.at[number],
                loc_of(*step),
            )

    def forward(step):
        number, at = ORDER.index(step), RELAYED.index(step)
        with scope(f"relay{step[0]}{step[2]}"):
            relay_copies[step].wait_recv()
        halo_copies[step] = start_copy(
            relay.at[at], recv.at[number], relay_send.at[at], halo_recv.at[number],
            loc_of(step[0], 0, step[2]),
        )

    def exchange(stage_number):
        for step in PLAN[stage_number][0]:
            if stage_number < 3 and step != ORDER[0]:
                gather(ORDER.index(step))
            send(step)
        for step in PLAN[stage_number][1]:
            forward(step)

    with scope("gather0"):
        gather(0)
    with scope("barrier"):
        pl.semaphore_wait(barrier, len(greeted) + jnp.where(z == 0, 0, NZ - 1))
    exchange(0)

    for to in ring:

        @pl.when((z == 0) | (to == 0))
        def _():
            signal(barrier, (xl * 4 + to, l))

    for number, where in enumerate(beside):
        signal(others_in.at[number], where)

    with scope("gather1"):
        exchange(1)

    with scope("hubpart"):
        loads[6].wait()
        upper = lax.broadcasted_iota(jnp.int32, (128, 128), 0) % 8 < 4
        for start in range(0, HUBS, 128):
            rows = mm(hub[start : start + 128, :], fhi[...])
            left, right = rows[:, :128], rows[:, 128:]
            part[0, start : start + 128, :] = jnp.where(upper, left, pltpu.roll(right, 4, 0))
            part[1, start : start + 128, :] = jnp.where(upper, pltpu.roll(left, 124, 0), right)
        pair_copy = pltpu.make_async_remote_copy(
            src_ref=part.at[1 - c],
            dst_ref=part_in,
            send_sem=a_sem.at[0],
            recv_sem=a_sem.at[1],
            device_id=(g, loc_of(0, 0, 1)),
            device_id_type=MESH,
        )
        pair_copy.start()

    with scope("gather2"):
        exchange(2)
        for number in range(sum(len(sends) for sends, _ in PLAN[:3]), len(ORDER)):
            gather(number)

    with scope("a_to_b"):
        pair_copy.wait_recv()
        pair_sum[...] = (part[pl.ds(c, 1)][0] + part_in[...]).reshape(NXL, NZ, 64, 128)
        z_copies = []

        @pl.when(z == 0)
        def _():
            pl.semaphore_wait(barrier, NZ - 1)

        for dz in range(1, NZ):
            to = (z + dz) % NZ
            copy = pltpu.make_async_remote_copy(
                src_ref=pair_sum.at[:, to],
                dst_ref=z_in.at[dz - 1],
                send_sem=b_send.at[dz - 1],
                recv_sem=b_recv.at[dz - 1],
                device_id=(xl * 4 + to, l),
                device_id_type=MESH,
            )
            copy.start()
            z_copies.append(copy)


    with scope("marks"):
        loads[7].wait()
        loads[8].wait()
        slots, used = nbr[...], cnt[...]
        active = lax.broadcasted_iota(jnp.int32, (SLOTS, ROWS), 0) < used
        place = slots & (FIELD_ROWS - 1)
        one = jnp.where(active, jnp.left_shift(1, (slots >> 9) * FIELD_BITS), 0)
        inverse = jnp.broadcast_to(1.0 / used.astype(jnp.float32), (8, ROWS))
        for start in range(0, ROWS, 128):
            rows = slice(start, start + 128)
            marks[0, rows, :] = place[:, rows].T
            marks[1, rows, :] = one[:, rows].T
            recip[rows, :] = inverse[:, rows].T

    pool_lane = lax.broadcasted_iota(jnp.int32, (32, FIELD_ROWS), 1)

    def build(block, carry):
        rows = pl.ds(pl.multiple_of(block * 32, 32), 32)
        row_place, row_one = marks[0, rows, :], marks[1, rows, :]
        packed = jnp.zeros((32, FIELD_ROWS), jnp.int32)
        for k in range(SLOTS):
            packed = packed + jnp.where(
                row_place[:, k : k + 1] == pool_lane, row_one[:, k : k + 1], 0
            )
        for field in range(FIELDS):
            number = (packed >> (field * FIELD_BITS)) & (2**FIELD_BITS - 1)
            number = number.astype(jnp.float32).astype(jnp.bfloat16)
            if field < 2:
                links_own[2 * field, rows, :] = number[:, :256]
                links_own[2 * field + 1, rows, :] = number[:, 256:]
            else:
                for peer in range(4):
                    links = number[:, peer * SENT : (peer + 1) * SENT]
                    for half in range(2):
                        lanes = slice(half * SENT, (half + 1) * SENT)
                        links_far[(field - 2) * 4 + peer, rows, lanes] = links
        return carry

    exchange(3)
    with scope("build1"):
        lax.fori_loop(0, 8, build, 0)
    exchange(4)
    with scope("build2"):
        lax.fori_loop(8, 16, build, 0)
    exchange(5)
    with scope("build3"):
        lax.fori_loop(16, 24, build, 0)
    exchange(6)
    with scope("b_to_c"):
        for copy in z_copies:
            copy.wait_recv()
        for half in range(NXL):
            value = pair_sum[half, pl.ds(z, 1)][0]
            for dz in range(NZ - 1):
                value = value + z_in[dz, half]
            z_sum[half] = value.reshape(8, 8, 128)
        plane_copies = []
        for number in range(3):
            pl.semaphore_wait(others_in.at[number], 1)
        for dx in range(4):
            for dy in range(NY):
                if (dx, dy) == (0, 0):
                    continue
                tx, ty = (x + dx) % 4, (y + dy) % NY
                copy = pltpu.make_async_remote_copy(
                    src_ref=z_sum.at[tx % 2, ty * 2 + tx // 2],
                    dst_ref=plane_in.at[dx * 4 + dy],
                    send_sem=c_send.at[dx * 4 + dy],
                    recv_sem=c_recv.at[dx * 4 + dy],
                    device_id=plane_of(dx, dy),
                    device_id_type=MESH,
                )
                copy.start()
                plane_copies.append(copy)

    exchange(7)
    with scope("build4"):
        lax.fori_loop(24, 32, build, 0)
    exchange(8)

    with scope("hub_mark"):
        loads[9].wait()
        loads[10].wait()
        vertex = lax.broadcasted_iota(jnp.int32, (ROWS, 128), 0)
        lane = lax.broadcasted_iota(jnp.int32, (ROWS, 128), 1)
        mark = jnp.zeros((ROWS, 128), jnp.float32)
        for r in range(HUB_OWN):
            mark = jnp.where((vertex == slot[r]) & ((lane == r) | (lane == 4 + r)), 1.0, mark)
        hub_mark[...] = mark.astype(jnp.bfloat16)
        for start in range(0, ROWS, 256):
            rows = slice(start, start + 256)
            halves = [table[pl.ds(2 * start + half, 256, stride=2), :] for half in range(2)]
            value = jnp.concatenate(halves, axis=1)
            base[rows, :] = value + bias[...]
            ghi[rows, :], glo[rows, :] = split2(value)

    with scope("own"):
        for number in range(4):
            rows = slice(number * 256, (number + 1) * 256)
            value = mm(links_own[number], ghi[rows, :]) + mm(links_own[number], glo[rows, :])
            total[...] = value if number == 0 else total[...] + value

    def far(step):
        number = ORDER.index(step)
        dy, dx, dc = step
        if step != (0, 0, 0):
            with scope(f"wait{dy}{dx}{dc}"):
                halo_copies[step].wait_recv()
        peer = loc_from(dy, dx, dc)
        halves = [recv[number, :, half, :] for half in range(2)]
        high, low = split2(jnp.concatenate(halves, axis=1))
        return peer, jnp.concatenate([high, low], axis=0)

    def linked(peer, rows):
        return links_far[pl.ds(peer, 1), rows, :][0]

    def hub_rows():
        with scope("wait_c"):
            for copy in plane_copies:
                copy.wait_recv()
        with scope("hub_rows"):
            hub_tile = z_sum[pl.ds(xl, 1), pl.ds(y * 2 + xh, 1)][0, 0]
            for source in range(1, 16):
                hub_tile = hub_tile + plane_in[source]
            hub_own = weighed(jnp.concatenate([hub_tile, pltpu.roll(hub_tile, 4, 0)], axis=1))[1]
            upper = lax.broadcasted_iota(jnp.int32, (8, WIDTH), 0) < HUB_OWN
            high = hub_own.astype(jnp.bfloat16).astype(jnp.float32)
            both = jnp.where(upper, high, pltpu.roll(hub_own - high, 4, 0))
            hub_values = jnp.concatenate([both, jnp.zeros((120, WIDTH), jnp.float32)], axis=0)
            hub_values = hub_values.astype(jnp.bfloat16)
            base[...] += mm(hub_mark[...], hub_values)

    for kind, step in TAKE_ORDER:
        if kind == "hub":
            hub_rows()
        elif kind == "forward":
            forward(step)
        elif kind == "take":
            peer, values = far(step)
            with scope("take"):
                total[...] += mm(linked(peer, slice(None)), values)

    with scope("combine"):
        base[...] += total[...] * recip[:, 0:1]
        last = [step for kind, step in TAKE_ORDER if kind == "last"]
        for number, step in enumerate(last):
            last_links[number] = linked(loc_from(*step), slice(None))
    for number, step in enumerate(last):
        last_values[number] = far(step)[1]

    with scope("wait_send"):
        for copy in sent:
            copy.wait_send()
        pair_copy.wait_send()
        for copy in z_copies + plane_copies:
            copy.wait_send()


def finish(base, recip, last_links, last_values, out_hbm, out, out_sem):
    copies = []
    for start in range(0, ROWS, 256):
        rows = slice(start, start + 256)
        value = sum(mm(last_links[number, rows, :], last_values[number]) for number in range(LAST))
        out[rows, :] = jnp.maximum(base[rows, :] + value * recip[rows, 0:1], 0.0)
        piece = pl.ds(start, 256)
        copy = pltpu.make_async_copy(out.at[piece], out_hbm.at[piece], out_sem.at[start // 256])
        copy.start()
        copies.append(copy)
    for copy in copies:
        copy.wait()


def on_device(features, hub_block, hub_slot, neighbours, counts, halo_send, weight, bias):
    f32, bf16, i32 = jnp.float32, jnp.bfloat16, jnp.int32
    vmem, dma = pltpu.VMEM, pltpu.SemaphoreType.DMA
    handed = pl.pallas_call(
        kernel,
        out_shape=(
            jax.ShapeDtypeStruct((ROWS, WIDTH), f32),
            jax.ShapeDtypeStruct((ROWS, 8), f32),
            jax.ShapeDtypeStruct((LAST, ROWS, 2 * SENT), bf16),
            jax.ShapeDtypeStruct((LAST, 2 * SENT, WIDTH), bf16),
        ),
        in_specs=[pl.BlockSpec(memory_space=pltpu.HBM)] * 8,
        out_specs=(pl.BlockSpec(memory_space=pltpu.VMEM),) * 4,
        scratch_shapes=[
            vmem((ROWS, WIDTH), f32),
            vmem((HUBS, ROWS), bf16),
            pltpu.SMEM((HUB_OWN,), i32),
            vmem((SLOTS, ROWS), i32),
            vmem((1, ROWS), i32),
            pltpu.SMEM((16, SENT), i32),
            vmem((WIDTH, WIDTH), f32),
            vmem((1, WIDTH), f32),
            vmem((ROWS, WIDTH), bf16),
            vmem((2 * ROWS, 128), f32),
            vmem((ROWS, WIDTH), bf16),
            vmem((ROWS, WIDTH), bf16),
            vmem((16, SENT, 2, 128), f32),
            vmem((16, SENT, 2, 128), f32),
            vmem((6, SENT, 2, 128), f32),
            vmem((NC, HUBS, 128), f32),
            vmem((HUBS, 128), f32),
            vmem((NXL, NZ, 64, 128), f32),
            vmem((NZ - 1, NXL, 64, 128), f32),
            vmem((NXL, 8, 8, 128), f32),
            vmem((16, 8, 128), f32),
            vmem((2, ROWS, SLOTS), i32),
            vmem((ROWS, 128), bf16),
            vmem((4, ROWS, 256), bf16),
            vmem((16, ROWS, 2 * SENT), bf16),
            vmem((ROWS, WIDTH), f32),
            vmem((WIDTH, WIDTH), bf16),
            vmem((WIDTH, WIDTH), bf16),
            dma((11,)), dma((16,)), dma((16,)), dma((6,)), dma((6,)), dma((2,)),
            dma((3,)), dma((3,)), dma((16,)), dma((16,)), pltpu.SemaphoreType.REGULAR((3,)),
        ],
        compiler_params=pltpu.CompilerParams(
            collective_id=0, has_side_effects=True, vmem_limit_bytes=40 * 1024 * 1024
        ),
    )(
        *(
            pltpu.with_memory_space_constraint(array, pltpu.HBM)
            for array in (
                features, hub_block, hub_slot, neighbours.T, counts.reshape(1, -1), halo_send,
                weight, bias.reshape(1, -1),
            )
        )
    )
    return pl.pallas_call(
        finish,
        out_shape=jax.ShapeDtypeStruct((ROWS, WIDTH), f32),
        in_specs=[pl.BlockSpec(memory_space=pltpu.VMEM)] * 4,
        out_specs=pl.BlockSpec(memory_space=pl.ANY),
        scratch_shapes=[vmem((ROWS, WIDTH), f32), dma((4,))],
        compiler_params=pltpu.CompilerParams(vmem_limit_bytes=8 * 1024 * 1024),
    )(*handed)


def solution(mesh):
    in_specs = (
        P(("grp", "loc"), None),
        P(None, ("grp", "loc")),
        P(("grp", "loc")),
        P(("grp", "loc"), None),
        P(("grp", "loc")),
        P(("grp", "loc"), None),
        P(),
        P(),
    )
    out_specs = P(("grp", "loc"), None)
    return jax.shard_map(
        on_device, mesh=mesh, in_specs=in_specs, out_specs=out_specs, check_vma=False
    )
```

```python
import jax
import jax.numpy as jnp
from jax import lax
from jax.experimental import pallas as pl
from jax.experimental.pallas import tpu as pltpu
from jax.sharding import PartitionSpec as P

MESH = pl.DeviceIdType.MESH
NY, NXH, NC, NXL, NZ = 4, 2, 2, 2, 4
ROWS, WIDTH, SLOTS, SENT = 1024, 256, 16, 128
HUBS, HUB_OWN = 512, 4
FIELD_ROWS, FIELDS, FIELD_BITS = 512, 6, 5

PLAN = (
    (((2, 1, 0), ), ()),
    (((1, 0, 0), (2, 1, 1), (3, 0, 0), ), ()),
    (((1, 1, 0), (2, 0, 0), (3, 1, 0), (2, 0, 1), (1, 0, 1), (3, 0, 1), (0, 0, 1), (0, 0, 0), ), ()),
    (((1, 1, 1), (3, 1, 1), ), ()),
    ((), ((2, 1, 0), )),
    ((), ((2, 1, 1), )),
    ((), ()),
    (((0, 1, 0), (0, 1, 1), ), ()),
    ((), ((1, 1, 0), )),
)
TAKE_ORDER = (
    ("take", (0, 0, 0)), ("take", (0, 0, 1)), ("forward", (3, 1, 0)),
    ("take", (1, 0, 0)), ("take", (3, 0, 0)), ("take", (2, 0, 0)),
    ("forward", (1, 1, 1)), ("take", (2, 0, 1)), ("take", (1, 0, 1)),
    ("take", (3, 0, 1)), ("take", (2, 1, 0)), ("forward", (3, 1, 1)),
    ("take", (2, 1, 1)), ("take", (1, 1, 0)), ("hub", (0, 0, 0)),
    ("take", (0, 1, 0)), ("take", (3, 1, 0)), ("combine", (0, 0, 0)), ("take", (0, 1, 1)),
    ("last", (1, 1, 1)), ("last", (3, 1, 1)),
)


ORDER = tuple(step for sends, _ in PLAN for step in sends)
LAST = sum(kind == "last" for kind, _ in TAKE_ORDER)
RELAYED = tuple(step for step in ORDER if step[0] != 0 and step[1] != 0)


def split2(value):
    high = value.astype(jnp.bfloat16)
    low = (value - high.astype(jnp.float32)).astype(jnp.bfloat16)
    return high, low


def mm(left, right):
    return jnp.dot(left, right, preferred_element_type=jnp.float32)


def scope(name):
    return jax.named_scope(name)


def kernel(
    feat_hbm, hub_hbm, slot_hbm, nbr_hbm, cnt_hbm, halo_hbm, weight_hbm, bias_hbm,
    base, recip, last_links, last_values,
    feat, hub, slot, nbr, cnt, halo, weight, bias,
    fhi, table, ghi, glo, stage, recv, relay,
    part, part_in, pair_sum, z_in, z_sum, plane_in,
    marks, hub_mark, links_own, links_far, total, w_hi, w_lo,
    in_sem, halo_send, halo_recv, relay_send, relay_recv, a_sem, b_send, b_recv, c_send, c_recv, others_in,
):
    g, l = lax.axis_index("grp"), lax.axis_index("loc")
    y, xh, c = l // 4, (l // 2) % 2, l % 2
    xl, z = g // 4, g % 4
    x = xh * 2 + xl

    def loc_of(dy, dx, dc):
        return ((y + dy + 2 * c * dy) % NY) * 4 + ((xh + dx) % NXH) * 2 + (c + dc) % NC

    def loc_from(dy, dx, dc):
        source = (c + dc) % NC
        return ((y - dy - 2 * source * dy + 3 * NY) % NY) * 4 + ((xh + dx) % NXH) * 2 + source

    def plane_of(dx, dy):
        tx, ty = (x + dx) % 4, (y + dy) % NY
        return (tx % 2) * 4 + z, ty * 4 + (tx // 2) * 2 + c

    quarter = [pl.ds(start, 256) for start in range(0, ROWS, 256)]
    loads = []
    for number, (source, target) in enumerate((
        *((feat_hbm.at[q], feat.at[q]) for q in quarter), (weight_hbm, weight), (halo_hbm, halo),
        (hub_hbm, hub), (nbr_hbm, nbr), (cnt_hbm, cnt), (bias_hbm, bias), (slot_hbm, slot),
    )):
        copy = pltpu.make_async_copy(source, target, in_sem.at[number])
        copy.start()
        loads.append(copy)

    def signal(semaphore, where):
        pl.semaphore_signal(semaphore, inc=1, device_id=where, device_id_type=MESH)

    barrier = pltpu.get_barrier_semaphore()
    beside = (plane_of(1, 0), plane_of(3, 0), plane_of(2, 0))
    greeted = [(g, loc_of(*step)) for step in ORDER if step != (0, 0, 0) and step not in RELAYED]
    greeted += beside[:2]
    for where in greeted:
        signal(barrier, where)
    ring = [(z + dz) % NZ for dz in range(1, NZ)]
    for to in ring:

        @pl.when((z != 0) & (to != 0))
        def _():
            signal(barrier, (xl * 4 + to, l))

    with scope("inputs"):
        loads[4].wait()
        w_hi[...], w_lo[...] = split2(weight[...])
        for copy in loads[:4]:
            copy.wait()

    def weighed(value):
        high, low = split2(value)
        return high, mm(high, w_hi[...]) + mm(low, w_hi[...]) + mm(high, w_lo[...])

    with scope("fw"):
        for start in range(0, ROWS, 256):
            rows = slice(start, start + 256)
            fhi[rows, :], value = weighed(feat[rows, :])
            for half in range(2):
                table[pl.ds(2 * start + half, 256, stride=2), :] = value[:, half * 128 : (half + 1) * 128]
        loads[5].wait()

    halo_copies, relay_copies, sent = {}, {}, []

    by_row = table.reshape(ROWS, 2, 128)

    def gather(number):
        step = ORDER[number]
        peer = loc_of(*step)
        target = recv if step == (0, 0, 0) else stage
        for row in range(SENT):
            target[number, row] = by_row[halo[peer, row]]

    def start_copy(source, target, send_sem, recv_sem, where):
        copy = pltpu.make_async_remote_copy(
            src_ref=source, dst_ref=target, send_sem=send_sem, recv_sem=recv_sem,
            device_id=(g, where), device_id_type=MESH,
        )
        copy.start()
        sent.append(copy)
        return copy

    def send(step):
        number = ORDER.index(step)
        if step in RELAYED:
            at = RELAYED.index(step)
            relay_copies[step] = start_copy(
                stage.at[number], relay.at[at], halo_send.at[number], relay_recv.at[at],
                loc_of(0, 1, 0),
            )
        elif step != (0, 0, 0):
            halo_copies[step] = start_copy(
                stage.at[number], recv.at[number], halo_send.at[number], halo_recv.at[number],
                loc_of(*step),
            )

    def forward(step):
        number, at = ORDER.index(step), RELAYED.index(step)
        with scope(f"relay{step[0]}{step[2]}"):
            relay_copies[step].wait_recv()
        halo_copies[step] = start_copy(
            relay.at[at], recv.at[number], relay_send.at[at], halo_recv.at[number],
            loc_of(step[0], 0, step[2]),
        )

    def exchange(stage_number):
        for step in PLAN[stage_number][0]:
            if stage_number < 3 and step != ORDER[0]:
                gather(ORDER.index(step))
            send(step)
        for step in PLAN[stage_number][1]:
            forward(step)

    with scope("gather0"):
        gather(0)
    with scope("barrier"):
        pl.semaphore_wait(barrier, len(greeted) + jnp.where(z == 0, 0, NZ - 1))
    exchange(0)

    for to in ring:

        @pl.when((z == 0) | (to == 0))
        def _():
            signal(barrier, (xl * 4 + to, l))

    for number, where in enumerate(beside):
        signal(others_in.at[number], where)

    with scope("gather1"):
        exchange(1)

    with scope("hubpart"):
        loads[6].wait()
        upper = lax.broadcasted_iota(jnp.int32, (128, 128), 0) % 8 < 4
        for start in range(0, HUBS, 128):
            rows = mm(hub[start : start + 128, :], fhi[...])
            left, right = rows[:, :128], rows[:, 128:]
            part[0, start : start + 128, :] = jnp.where(upper, left, pltpu.roll(right, 4, 0))
            part[1, start : start + 128, :] = jnp.where(upper, pltpu.roll(left, 124, 0), right)
        pair_copy = pltpu.make_async_remote_copy(
            src_ref=part.at[1 - c],
            dst_ref=part_in,
            send_sem=a_sem.at[0],
            recv_sem=a_sem.at[1],
            device_id=(g, loc_of(0, 0, 1)),
            device_id_type=MESH,
        )
        pair_copy.start()

    with scope("gather2"):
        exchange(2)
        for number in range(sum(len(sends) for sends, _ in PLAN[:3]), len(ORDER)):
            gather(number)

    with scope("a_to_b"):
        pair_copy.wait_recv()
        pair_sum[...] = (part[pl.ds(c, 1)][0] + part_in[...]).reshape(NXL, NZ, 64, 128)
        z_copies = []

        @pl.when(z == 0)
        def _():
            pl.semaphore_wait(barrier, NZ - 1)

        for dz in range(1, NZ):
            to = (z + dz) % NZ
            copy = pltpu.make_async_remote_copy(
                src_ref=pair_sum.at[:, to],
                dst_ref=z_in.at[dz - 1],
                send_sem=b_send.at[dz - 1],
                recv_sem=b_recv.at[dz - 1],
                device_id=(xl * 4 + to, l),
                device_id_type=MESH,
            )
            copy.start()
            z_copies.append(copy)


    with scope("marks"):
        loads[7].wait()
        loads[8].wait()
        slots, used = nbr[...], cnt[...]
        active = lax.broadcasted_iota(jnp.int32, (SLOTS, ROWS), 0) < used
        place = slots & (FIELD_ROWS - 1)
        one = jnp.where(active, jnp.left_shift(1, (slots >> 9) * FIELD_BITS), 0)
        inverse = jnp.broadcast_to(1.0 / used.astype(jnp.float32), (8, ROWS))
        for start in range(0, ROWS, 128):
            rows = slice(start, start + 128)
            marks[0, rows, :] = place[:, rows].T
            marks[1, rows, :] = one[:, rows].T
            recip[rows, :] = inverse[:, rows].T

    pool_lane = lax.broadcasted_iota(jnp.int32, (32, FIELD_ROWS), 1)

    def build(block, carry):
        rows = pl.ds(pl.multiple_of(block * 32, 32), 32)
        row_place, row_one = marks[0, rows, :], marks[1, rows, :]
        packed = jnp.zeros((32, FIELD_ROWS), jnp.int32)
        for k in range(SLOTS):
            packed = packed + jnp.where(
                row_place[:, k : k + 1] == pool_lane, row_one[:, k : k + 1], 0
            )
        for field in range(FIELDS):
            number = (packed >> (field * FIELD_BITS)) & (2**FIELD_BITS - 1)
            number = number.astype(jnp.float32).astype(jnp.bfloat16)
            if field < 2:
                links_own[2 * field, rows, :] = number[:, :256]
                links_own[2 * field + 1, rows, :] = number[:, 256:]
            else:
                for peer in range(4):
                    links = number[:, peer * SENT : (peer + 1) * SENT]
                    for half in range(2):
                        lanes = slice(half * SENT, (half + 1) * SENT)
                        links_far[(field - 2) * 4 + peer, rows, lanes] = links
        return carry

    exchange(3)
    with scope("build1"):
        lax.fori_loop(0, 8, build, 0)
    exchange(4)
    with scope("build2"):
        lax.fori_loop(8, 16, build, 0)
    exchange(5)
    with scope("build3"):
        lax.fori_loop(16, 24, build, 0)
    exchange(6)
    with scope("b_to_c"):
        for copy in z_copies:
            copy.wait_recv()
        for half in range(NXL):
            value = pair_sum[half, pl.ds(z, 1)][0]
            for dz in range(NZ - 1):
                value = value + z_in[dz, half]
            z_sum[half] = value.reshape(8, 8, 128)
        plane_copies = []
        for number in range(3):
            pl.semaphore_wait(others_in.at[number], 1)
        for dx in range(4):
            for dy in range(NY):
                if (dx, dy) == (0, 0):
                    continue
                tx, ty = (x + dx) % 4, (y + dy) % NY
                copy = pltpu.make_async_remote_copy(
                    src_ref=z_sum.at[tx % 2, ty * 2 + tx // 2],
                    dst_ref=plane_in.at[dx * 4 + dy],
                    send_sem=c_send.at[dx * 4 + dy],
                    recv_sem=c_recv.at[dx * 4 + dy],
                    device_id=plane_of(dx, dy),
                    device_id_type=MESH,
                )
                copy.start()
                plane_copies.append(copy)

    exchange(7)
    with scope("build4"):
        lax.fori_loop(24, 32, build, 0)
    exchange(8)

    with scope("hub_mark"):
        loads[9].wait()
        loads[10].wait()
        vertex = lax.broadcasted_iota(jnp.int32, (ROWS, 128), 0)
        lane = lax.broadcasted_iota(jnp.int32, (ROWS, 128), 1)
        mark = jnp.zeros((ROWS, 128), jnp.float32)
        for r in range(HUB_OWN):
            mark = jnp.where((vertex == slot[r]) & ((lane == r) | (lane == 4 + r)), 1.0, mark)
        hub_mark[...] = mark.astype(jnp.bfloat16)
        for start in range(0, ROWS, 256):
            rows = slice(start, start + 256)
            halves = [table[pl.ds(2 * start + half, 256, stride=2), :] for half in range(2)]
            value = jnp.concatenate(halves, axis=1)
            base[rows, :] = value + bias[...]
            ghi[rows, :], glo[rows, :] = split2(value)

    with scope("own"):
        for number in range(4):
            rows = slice(number * 256, (number + 1) * 256)
            value = mm(links_own[number], ghi[rows, :]) + mm(links_own[number], glo[rows, :])
            total[...] = value if number == 0 else total[...] + value

    def far(step):
        number = ORDER.index(step)
        dy, dx, dc = step
        if step != (0, 0, 0):
            with scope(f"wait{dy}{dx}{dc}"):
                halo_copies[step].wait_recv()
        peer = loc_from(dy, dx, dc)
        halves = [recv[number, :, half, :] for half in range(2)]
        high, low = split2(jnp.concatenate(halves, axis=1))
        return peer, jnp.concatenate([high, low], axis=0)

    def linked(peer, rows):
        return links_far[pl.ds(peer, 1), rows, :][0]

    def hub_rows():
        with scope("wait_c"):
            for copy in plane_copies:
                copy.wait_recv()
        with scope("hub_rows"):
            hub_tile = z_sum[pl.ds(xl, 1), pl.ds(y * 2 + xh, 1)][0, 0]
            for source in range(1, 16):
                hub_tile = hub_tile + plane_in[source]
            hub_own = weighed(jnp.concatenate([hub_tile, pltpu.roll(hub_tile, 4, 0)], axis=1))[1]
            upper = lax.broadcasted_iota(jnp.int32, (8, WIDTH), 0) < HUB_OWN
            high = hub_own.astype(jnp.bfloat16).astype(jnp.float32)
            both = jnp.where(upper, high, pltpu.roll(hub_own - high, 4, 0))
            hub_values = jnp.concatenate([both, jnp.zeros((120, WIDTH), jnp.float32)], axis=0)
            hub_values = hub_values.astype(jnp.bfloat16)
            base[...] += mm(hub_mark[...], hub_values)

    last = [step for kind, step in TAKE_ORDER if kind == "last"]
    combined = False
    for kind, step in TAKE_ORDER:
        if kind == "hub":
            hub_rows()
        elif kind == "forward":
            forward(step)
        elif kind == "combine":
            with scope("combine"):
                base[...] += total[...] * recip[:, 0:1]
                for number, later in enumerate(last):
                    last_links[number] = linked(loc_from(*later), slice(None))
            combined = True
        elif kind == "take":
            peer, values = far(step)
            with scope("take"):
                value = mm(linked(peer, slice(None)), values)
                if combined:
                    base[...] += value * recip[:, 0:1]
                else:
                    total[...] += value

    for number, step in enumerate(last):
        last_values[number] = far(step)[1]

    with scope("wait_send"):
        for copy in sent:
            copy.wait_send()
        pair_copy.wait_send()
        for copy in z_copies + plane_copies:
            copy.wait_send()


def finish(base, recip, last_links, last_values, out_hbm, out, out_sem):
    copies = []
    for start in range(0, ROWS, 256):
        rows = slice(start, start + 256)
        value = sum(mm(last_links[number, rows, :], last_values[number]) for number in range(LAST))
        out[rows, :] = jnp.maximum(base[rows, :] + value * recip[rows, 0:1], 0.0)
        piece = pl.ds(start, 256)
        copy = pltpu.make_async_copy(out.at[piece], out_hbm.at[piece], out_sem.at[start // 256])
        copy.start()
        copies.append(copy)
    for copy in copies:
        copy.wait()


def on_device(features, hub_block, hub_slot, neighbours, counts, halo_send, weight, bias):
    f32, bf16, i32 = jnp.float32, jnp.bfloat16, jnp.int32
    vmem, dma = pltpu.VMEM, pltpu.SemaphoreType.DMA
    handed = pl.pallas_call(
        kernel,
        out_shape=(
            jax.ShapeDtypeStruct((ROWS, WIDTH), f32),
            jax.ShapeDtypeStruct((ROWS, 8), f32),
            jax.ShapeDtypeStruct((LAST, ROWS, 2 * SENT), bf16),
            jax.ShapeDtypeStruct((LAST, 2 * SENT, WIDTH), bf16),
        ),
        in_specs=[pl.BlockSpec(memory_space=pltpu.HBM)] * 8,
        out_specs=(pl.BlockSpec(memory_space=pltpu.VMEM),) * 4,
        scratch_shapes=[
            vmem((ROWS, WIDTH), f32),
            vmem((HUBS, ROWS), bf16),
            pltpu.SMEM((HUB_OWN,), i32),
            vmem((SLOTS, ROWS), i32),
            vmem((1, ROWS), i32),
            pltpu.SMEM((16, SENT), i32),
            vmem((WIDTH, WIDTH), f32),
            vmem((1, WIDTH), f32),
            vmem((ROWS, WIDTH), bf16),
            vmem((2 * ROWS, 128), f32),
            vmem((ROWS, WIDTH), bf16),
            vmem((ROWS, WIDTH), bf16),
            vmem((16, SENT, 2, 128), f32),
            vmem((16, SENT, 2, 128), f32),
            vmem((6, SENT, 2, 128), f32),
            vmem((NC, HUBS, 128), f32),
            vmem((HUBS, 128), f32),
            vmem((NXL, NZ, 64, 128), f32),
            vmem((NZ - 1, NXL, 64, 128), f32),
            vmem((NXL, 8, 8, 128), f32),
            vmem((16, 8, 128), f32),
            vmem((2, ROWS, SLOTS), i32),
            vmem((ROWS, 128), bf16),
            vmem((4, ROWS, 256), bf16),
            vmem((16, ROWS, 2 * SENT), bf16),
            vmem((ROWS, WIDTH), f32),
            vmem((WIDTH, WIDTH), bf16),
            vmem((WIDTH, WIDTH), bf16),
            dma((11,)), dma((16,)), dma((16,)), dma((6,)), dma((6,)), dma((2,)),
            dma((3,)), dma((3,)), dma((16,)), dma((16,)), pltpu.SemaphoreType.REGULAR((3,)),
        ],
        compiler_params=pltpu.CompilerParams(
            collective_id=0, has_side_effects=True, vmem_limit_bytes=40 * 1024 * 1024
        ),
    )(
        *(
            pltpu.with_memory_space_constraint(array, pltpu.HBM)
            for array in (
                features, hub_block, hub_slot, neighbours.T, counts.reshape(1, -1), halo_send,
                weight, bias.reshape(1, -1),
            )
        )
    )
    return pl.pallas_call(
        finish,
        out_shape=jax.ShapeDtypeStruct((ROWS, WIDTH), f32),
        in_specs=[pl.BlockSpec(memory_space=pltpu.VMEM)] * 4,
        out_specs=pl.BlockSpec(memory_space=pl.ANY),
        scratch_shapes=[vmem((ROWS, WIDTH), f32), dma((4,))],
        compiler_params=pltpu.CompilerParams(vmem_limit_bytes=8 * 1024 * 1024),
    )(*handed)


def solution(mesh):
    in_specs = (
        P(("grp", "loc"), None),
        P(None, ("grp", "loc")),
        P(("grp", "loc")),
        P(("grp", "loc"), None),
        P(("grp", "loc")),
        P(("grp", "loc"), None),
        P(),
        P(),
    )
    out_specs = P(("grp", "loc"), None)
    return jax.shard_map(
        on_device, mesh=mesh, in_specs=in_specs, out_specs=out_specs, check_vma=False
    )
```

```python
import jax
import jax.numpy as jnp
from jax import lax
from jax.experimental import pallas as pl
from jax.experimental.pallas import tpu as pltpu
from jax.sharding import PartitionSpec as P

MESH = pl.DeviceIdType.MESH
NY, NXH, NC, NXL, NZ = 4, 2, 2, 2, 4
ROWS, WIDTH, SLOTS, SENT = 1024, 256, 16, 128
HUBS, HUB_OWN = 512, 4
FIELD_ROWS, FIELDS, FIELD_BITS = 512, 6, 5

PLAN = (
    (((2, 1, 0), ), ()),
    (((1, 0, 0), (2, 1, 1), (3, 0, 0), ), ()),
    (((1, 1, 0), (2, 0, 0), (3, 1, 0), (2, 0, 1), (1, 0, 1), (3, 0, 1), (0, 0, 1), (0, 0, 0), ), ()),
    (((1, 1, 1), (3, 1, 1), ), ()),
    ((), ((2, 1, 0), )),
    ((), ((2, 1, 1), )),
    ((), ()),
    (((0, 1, 0), (0, 1, 1), ), ()),
    ((), ((1, 1, 0), )),
)
TAKE_ORDER = (
    ("take", (0, 0, 0)), ("take", (0, 0, 1)), ("forward", (3, 1, 0)),
    ("take", (1, 0, 0)), ("take", (3, 0, 0)), ("take", (2, 0, 0)),
    ("forward", (1, 1, 1)), ("take", (2, 0, 1)), ("take", (1, 0, 1)),
    ("take", (3, 0, 1)), ("take", (2, 1, 0)), ("forward", (3, 1, 1)),
    ("take", (2, 1, 1)), ("take", (1, 1, 0)), ("hub", (0, 0, 0)),
    ("take", (0, 1, 0)), ("take", (3, 1, 0)), ("combine", (0, 0, 0)), ("take", (0, 1, 1)),
    ("take", (3, 1, 1)), ("last", (1, 1, 1)),
)


ORDER = tuple(step for sends, _ in PLAN for step in sends)
LAST = sum(kind == "last" for kind, _ in TAKE_ORDER)
RELAYED = tuple(step for step in ORDER if step[0] != 0 and step[1] != 0)


def split2(value):
    high = value.astype(jnp.bfloat16)
    low = (value - high.astype(jnp.float32)).astype(jnp.bfloat16)
    return high, low


def mm(left, right):
    return jnp.dot(left, right, preferred_element_type=jnp.float32)


def scope(name):
    return jax.named_scope(name)


def kernel(
    feat_hbm, hub_hbm, slot_hbm, nbr_hbm, cnt_hbm, halo_hbm, weight_hbm, bias_hbm,
    base, recip, last_links, last_values,
    feat, hub, slot, nbr, cnt, halo, weight, bias,
    fhi, table, ghi, glo, stage, recv, relay,
    part, part_in, pair_sum, z_in, z_sum, plane_in,
    marks, hub_mark, links_own, links_far, total, w_hi, w_lo,
    in_sem, halo_send, halo_recv, relay_send, relay_recv, a_sem, b_send, b_recv, c_send, c_recv, others_in,
):
    g, l = lax.axis_index("grp"), lax.axis_index("loc")
    y, xh, c = l // 4, (l // 2) % 2, l % 2
    xl, z = g // 4, g % 4
    x = xh * 2 + xl

    def loc_of(dy, dx, dc):
        return ((y + dy + 2 * c * dy) % NY) * 4 + ((xh + dx) % NXH) * 2 + (c + dc) % NC

    def loc_from(dy, dx, dc):
        source = (c + dc) % NC
        return ((y - dy - 2 * source * dy + 3 * NY) % NY) * 4 + ((xh + dx) % NXH) * 2 + source

    def plane_of(dx, dy):
        tx, ty = (x + dx) % 4, (y + dy) % NY
        return (tx % 2) * 4 + z, ty * 4 + (tx // 2) * 2 + c

    quarter = [pl.ds(start, 256) for start in range(0, ROWS, 256)]
    loads = []
    for number, (source, target) in enumerate((
        *((feat_hbm.at[q], feat.at[q]) for q in quarter), (weight_hbm, weight), (halo_hbm, halo),
        (hub_hbm, hub), (nbr_hbm, nbr), (cnt_hbm, cnt), (bias_hbm, bias), (slot_hbm, slot),
    )):
        copy = pltpu.make_async_copy(source, target, in_sem.at[number])
        copy.start()
        loads.append(copy)

    def signal(semaphore, where):
        pl.semaphore_signal(semaphore, inc=1, device_id=where, device_id_type=MESH)

    barrier = pltpu.get_barrier_semaphore()
    beside = (plane_of(1, 0), plane_of(3, 0), plane_of(2, 0))
    greeted = [(g, loc_of(*step)) for step in ORDER if step != (0, 0, 0) and step not in RELAYED]
    greeted += beside[:2]
    for where in greeted:
        signal(barrier, where)
    ring = [(z + dz) % NZ for dz in range(1, NZ)]
    for to in ring:

        @pl.when((z != 0) & (to != 0))
        def _():
            signal(barrier, (xl * 4 + to, l))

    with scope("inputs"):
        loads[4].wait()
        w_hi[...], w_lo[...] = split2(weight[...])
        for copy in loads[:4]:
            copy.wait()

    def weighed(value):
        high, low = split2(value)
        return high, mm(high, w_hi[...]) + mm(low, w_hi[...]) + mm(high, w_lo[...])

    with scope("fw"):
        for start in range(0, ROWS, 256):
            rows = slice(start, start + 256)
            fhi[rows, :], value = weighed(feat[rows, :])
            for half in range(2):
                table[pl.ds(2 * start + half, 256, stride=2), :] = value[:, half * 128 : (half + 1) * 128]
        loads[5].wait()

    halo_copies, relay_copies, sent = {}, {}, []

    by_row = table.reshape(ROWS, 2, 128)

    def gather(number):
        step = ORDER[number]
        peer = loc_of(*step)
        target = recv if step == (0, 0, 0) else stage
        for row in range(SENT):
            target[number, row] = by_row[halo[peer, row]]

    def start_copy(source, target, send_sem, recv_sem, where):
        copy = pltpu.make_async_remote_copy(
            src_ref=source, dst_ref=target, send_sem=send_sem, recv_sem=recv_sem,
            device_id=(g, where), device_id_type=MESH,
        )
        copy.start()
        sent.append(copy)
        return copy

    def send(step):
        number = ORDER.index(step)
        if step in RELAYED:
            at = RELAYED.index(step)
            relay_copies[step] = start_copy(
                stage.at[number], relay.at[at], halo_send.at[number], relay_recv.at[at],
                loc_of(0, 1, 0),
            )
        elif step != (0, 0, 0):
            halo_copies[step] = start_copy(
                stage.at[number], recv.at[number], halo_send.at[number], halo_recv.at[number],
                loc_of(*step),
            )

    def forward(step):
        number, at = ORDER.index(step), RELAYED.index(step)
        with scope(f"relay{step[0]}{step[2]}"):
            relay_copies[step].wait_recv()
        halo_copies[step] = start_copy(
            relay.at[at], recv.at[number], relay_send.at[at], halo_recv.at[number],
            loc_of(step[0], 0, step[2]),
        )

    def exchange(stage_number):
        for step in PLAN[stage_number][0]:
            if stage_number < 3 and step != ORDER[0]:
                gather(ORDER.index(step))
            send(step)
        for step in PLAN[stage_number][1]:
            forward(step)

    with scope("gather0"):
        gather(0)
    with scope("barrier"):
        pl.semaphore_wait(barrier, len(greeted) + jnp.where(z == 0, 0, NZ - 1))
    exchange(0)

    for to in ring:

        @pl.when((z == 0) | (to == 0))
        def _():
            signal(barrier, (xl * 4 + to, l))

    for number, where in enumerate(beside):
        signal(others_in.at[number], where)

    with scope("gather1"):
        exchange(1)

    with scope("hubpart"):
        loads[6].wait()
        upper = lax.broadcasted_iota(jnp.int32, (128, 128), 0) % 8 < 4
        for start in range(0, HUBS, 128):
            rows = mm(hub[start : start + 128, :], fhi[...])
            left, right = rows[:, :128], rows[:, 128:]
            part[0, start : start + 128, :] = jnp.where(upper, left, pltpu.roll(right, 4, 0))
            part[1, start : start + 128, :] = jnp.where(upper, pltpu.roll(left, 124, 0), right)
        pair_copy = pltpu.make_async_remote_copy(
            src_ref=part.at[1 - c],
            dst_ref=part_in,
            send_sem=a_sem.at[0],
            recv_sem=a_sem.at[1],
            device_id=(g, loc_of(0, 0, 1)),
            device_id_type=MESH,
        )
        pair_copy.start()

    with scope("gather2"):
        exchange(2)
        for number in range(sum(len(sends) for sends, _ in PLAN[:3]), len(ORDER)):
            gather(number)

    with scope("a_to_b"):
        pair_copy.wait_recv()
        pair_sum[...] = (part[pl.ds(c, 1)][0] + part_in[...]).reshape(NXL, NZ, 64, 128)
        z_copies = []

        @pl.when(z == 0)
        def _():
            pl.semaphore_wait(barrier, NZ - 1)

        for dz in range(1, NZ):
            to = (z + dz) % NZ
            copy = pltpu.make_async_remote_copy(
                src_ref=pair_sum.at[:, to],
                dst_ref=z_in.at[dz - 1],
                send_sem=b_send.at[dz - 1],
                recv_sem=b_recv.at[dz - 1],
                device_id=(xl * 4 + to, l),
                device_id_type=MESH,
            )
            copy.start()
            z_copies.append(copy)


    with scope("marks"):
        loads[7].wait()
        loads[8].wait()
        slots, used = nbr[...], cnt[...]
        active = lax.broadcasted_iota(jnp.int32, (SLOTS, ROWS), 0) < used
        place = slots & (FIELD_ROWS - 1)
        one = jnp.where(active, jnp.left_shift(1, (slots >> 9) * FIELD_BITS), 0)
        inverse = jnp.broadcast_to(1.0 / used.astype(jnp.float32), (8, ROWS))
        for start in range(0, ROWS, 128):
            rows = slice(start, start + 128)
            marks[0, rows, :] = place[:, rows].T
            marks[1, rows, :] = one[:, rows].T
            recip[rows, :] = inverse[:, rows].T

    pool_lane = lax.broadcasted_iota(jnp.int32, (32, FIELD_ROWS), 1)

    def build(block, carry):
        rows = pl.ds(pl.multiple_of(block * 32, 32), 32)
        row_place, row_one = marks[0, rows, :], marks[1, rows, :]
        packed = jnp.zeros((32, FIELD_ROWS), jnp.int32)
        for k in range(SLOTS):
            packed = packed + jnp.where(
                row_place[:, k : k + 1] == pool_lane, row_one[:, k : k + 1], 0
            )
        for field in range(FIELDS):
            number = (packed >> (field * FIELD_BITS)) & (2**FIELD_BITS - 1)
            number = number.astype(jnp.float32).astype(jnp.bfloat16)
            if field < 2:
                links_own[2 * field, rows, :] = number[:, :256]
                links_own[2 * field + 1, rows, :] = number[:, 256:]
            else:
                for peer in range(4):
                    links = number[:, peer * SENT : (peer + 1) * SENT]
                    for half in range(2):
                        lanes = slice(half * SENT, (half + 1) * SENT)
                        links_far[(field - 2) * 4 + peer, rows, lanes] = links
        return carry

    exchange(3)
    with scope("build1"):
        lax.fori_loop(0, 8, build, 0)
    exchange(4)
    with scope("build2"):
        lax.fori_loop(8, 16, build, 0)
    exchange(5)
    with scope("build3"):
        lax.fori_loop(16, 24, build, 0)
    exchange(6)
    with scope("b_to_c"):
        for copy in z_copies:
            copy.wait_recv()
        for half in range(NXL):
            value = pair_sum[half, pl.ds(z, 1)][0]
            for dz in range(NZ - 1):
                value = value + z_in[dz, half]
            z_sum[half] = value.reshape(8, 8, 128)
        plane_copies = []
        for number in range(3):
            pl.semaphore_wait(others_in.at[number], 1)
        for dx in range(4):
            for dy in range(NY):
                if (dx, dy) == (0, 0):
                    continue
                tx, ty = (x + dx) % 4, (y + dy) % NY
                copy = pltpu.make_async_remote_copy(
                    src_ref=z_sum.at[tx % 2, ty * 2 + tx // 2],
                    dst_ref=plane_in.at[dx * 4 + dy],
                    send_sem=c_send.at[dx * 4 + dy],
                    recv_sem=c_recv.at[dx * 4 + dy],
                    device_id=plane_of(dx, dy),
                    device_id_type=MESH,
                )
                copy.start()
                plane_copies.append(copy)

    exchange(7)
    with scope("build4"):
        lax.fori_loop(24, 32, build, 0)
    exchange(8)

    with scope("hub_mark"):
        loads[9].wait()
        loads[10].wait()
        vertex = lax.broadcasted_iota(jnp.int32, (ROWS, 128), 0)
        lane = lax.broadcasted_iota(jnp.int32, (ROWS, 128), 1)
        mark = jnp.zeros((ROWS, 128), jnp.float32)
        for r in range(HUB_OWN):
            mark = jnp.where((vertex == slot[r]) & ((lane == r) | (lane == 4 + r)), 1.0, mark)
        hub_mark[...] = mark.astype(jnp.bfloat16)
        for start in range(0, ROWS, 256):
            rows = slice(start, start + 256)
            halves = [table[pl.ds(2 * start + half, 256, stride=2), :] for half in range(2)]
            value = jnp.concatenate(halves, axis=1)
            base[rows, :] = value + bias[...]
            ghi[rows, :], glo[rows, :] = split2(value)

    with scope("own"):
        for number in range(4):
            rows = slice(number * 256, (number + 1) * 256)
            value = mm(links_own[number], ghi[rows, :]) + mm(links_own[number], glo[rows, :])
            total[...] = value if number == 0 else total[...] + value

    def far(step):
        number = ORDER.index(step)
        dy, dx, dc = step
        if step != (0, 0, 0):
            with scope(f"wait{dy}{dx}{dc}"):
                halo_copies[step].wait_recv()
        peer = loc_from(dy, dx, dc)
        halves = [recv[number, :, half, :] for half in range(2)]
        high, low = split2(jnp.concatenate(halves, axis=1))
        return peer, jnp.concatenate([high, low], axis=0)

    def linked(peer, rows):
        return links_far[pl.ds(peer, 1), rows, :][0]

    def hub_rows():
        with scope("wait_c"):
            for copy in plane_copies:
                copy.wait_recv()
        with scope("hub_rows"):
            hub_tile = z_sum[pl.ds(xl, 1), pl.ds(y * 2 + xh, 1)][0, 0]
            for source in range(1, 16):
                hub_tile = hub_tile + plane_in[source]
            hub_own = weighed(jnp.concatenate([hub_tile, pltpu.roll(hub_tile, 4, 0)], axis=1))[1]
            upper = lax.broadcasted_iota(jnp.int32, (8, WIDTH), 0) < HUB_OWN
            high = hub_own.astype(jnp.bfloat16).astype(jnp.float32)
            both = jnp.where(upper, high, pltpu.roll(hub_own - high, 4, 0))
            hub_values = jnp.concatenate([both, jnp.zeros((120, WIDTH), jnp.float32)], axis=0)
            hub_values = hub_values.astype(jnp.bfloat16)
            base[...] += mm(hub_mark[...], hub_values)

    last = [step for kind, step in TAKE_ORDER if kind == "last"]
    combined = False
    for kind, step in TAKE_ORDER:
        if kind == "hub":
            hub_rows()
        elif kind == "forward":
            forward(step)
        elif kind == "combine":
            with scope("combine"):
                base[...] += total[...] * recip[:, 0:1]
                for number, later in enumerate(last):
                    last_links[number] = linked(loc_from(*later), slice(None))
            combined = True
        elif kind == "take":
            peer, values = far(step)
            with scope("take"):
                value = mm(linked(peer, slice(None)), values)
                if combined:
                    base[...] += value * recip[:, 0:1]
                else:
                    total[...] += value

    for number, step in enumerate(last):
        last_values[number] = far(step)[1]

    with scope("wait_send"):
        for copy in sent:
            copy.wait_send()
        pair_copy.wait_send()
        for copy in z_copies + plane_copies:
            copy.wait_send()


def finish(base, recip, last_links, last_values, out_hbm, out, out_sem):
    copies = []
    for start in range(0, ROWS, 256):
        rows = slice(start, start + 256)
        value = sum(mm(last_links[number, rows, :], last_values[number]) for number in range(LAST))
        out[rows, :] = jnp.maximum(base[rows, :] + value * recip[rows, 0:1], 0.0)
        piece = pl.ds(start, 256)
        copy = pltpu.make_async_copy(out.at[piece], out_hbm.at[piece], out_sem.at[start // 256])
        copy.start()
        copies.append(copy)
    for copy in copies:
        copy.wait()


def on_device(features, hub_block, hub_slot, neighbours, counts, halo_send, weight, bias):
    f32, bf16, i32 = jnp.float32, jnp.bfloat16, jnp.int32
    vmem, dma = pltpu.VMEM, pltpu.SemaphoreType.DMA
    handed = pl.pallas_call(
        kernel,
        out_shape=(
            jax.ShapeDtypeStruct((ROWS, WIDTH), f32),
            jax.ShapeDtypeStruct((ROWS, 8), f32),
            jax.ShapeDtypeStruct((LAST, ROWS, 2 * SENT), bf16),
            jax.ShapeDtypeStruct((LAST, 2 * SENT, WIDTH), bf16),
        ),
        in_specs=[pl.BlockSpec(memory_space=pltpu.HBM)] * 8,
        out_specs=(pl.BlockSpec(memory_space=pltpu.VMEM),) * 4,
        scratch_shapes=[
            vmem((ROWS, WIDTH), f32),
            vmem((HUBS, ROWS), bf16),
            pltpu.SMEM((HUB_OWN,), i32),
            vmem((SLOTS, ROWS), i32),
            vmem((1, ROWS), i32),
            pltpu.SMEM((16, SENT), i32),
            vmem((WIDTH, WIDTH), f32),
            vmem((1, WIDTH), f32),
            vmem((ROWS, WIDTH), bf16),
            vmem((2 * ROWS, 128), f32),
            vmem((ROWS, WIDTH), bf16),
            vmem((ROWS, WIDTH), bf16),
            vmem((16, SENT, 2, 128), f32),
            vmem((16, SENT, 2, 128), f32),
            vmem((6, SENT, 2, 128), f32),
            vmem((NC, HUBS, 128), f32),
            vmem((HUBS, 128), f32),
            vmem((NXL, NZ, 64, 128), f32),
            vmem((NZ - 1, NXL, 64, 128), f32),
            vmem((NXL, 8, 8, 128), f32),
            vmem((16, 8, 128), f32),
            vmem((2, ROWS, SLOTS), i32),
            vmem((ROWS, 128), bf16),
            vmem((4, ROWS, 256), bf16),
            vmem((16, ROWS, 2 * SENT), bf16),
            vmem((ROWS, WIDTH), f32),
            vmem((WIDTH, WIDTH), bf16),
            vmem((WIDTH, WIDTH), bf16),
            dma((11,)), dma((16,)), dma((16,)), dma((6,)), dma((6,)), dma((2,)),
            dma((3,)), dma((3,)), dma((16,)), dma((16,)), pltpu.SemaphoreType.REGULAR((3,)),
        ],
        compiler_params=pltpu.CompilerParams(
            collective_id=0, has_side_effects=True, vmem_limit_bytes=40 * 1024 * 1024
        ),
    )(
        *(
            pltpu.with_memory_space_constraint(array, pltpu.HBM)
            for array in (
                features, hub_block, hub_slot, neighbours.T, counts.reshape(1, -1), halo_send,
                weight, bias.reshape(1, -1),
            )
        )
    )
    return pl.pallas_call(
        finish,
        out_shape=jax.ShapeDtypeStruct((ROWS, WIDTH), f32),
        in_specs=[pl.BlockSpec(memory_space=pltpu.VMEM)] * 4,
        out_specs=pl.BlockSpec(memory_space=pl.ANY),
        scratch_shapes=[vmem((ROWS, WIDTH), f32), dma((4,))],
        compiler_params=pltpu.CompilerParams(vmem_limit_bytes=8 * 1024 * 1024),
    )(*handed)


def solution(mesh):
    in_specs = (
        P(("grp", "loc"), None),
        P(None, ("grp", "loc")),
        P(("grp", "loc")),
        P(("grp", "loc"), None),
        P(("grp", "loc")),
        P(("grp", "loc"), None),
        P(),
        P(),
    )
    out_specs = P(("grp", "loc"), None)
    return jax.shard_map(
        on_device, mesh=mesh, in_specs=in_specs, out_specs=out_specs, check_vma=False
    )
```
